256 devices in a mesh: task: 8 (over y, core), col: 32 (over z, x).
Axes of the slice: x: 4, y: 4, z: 8, core: 2. Of those that a mesh axis runs over, the one named last changes fastest.
Arguments:
- layer_inputs: bfloat16 [8, 1024, 8192], P('task', None, 'col'), may hold values from -6 to 6
- queries: bfloat16 [8, 1024, 8192], P('task', None, 'col'), may hold values from -1000 to 1000, as said below
- key_values: bfloat16 [8, 1024, 2048], P('task', 'col'), may hold values from -8 to 8, as said below
- out_grads: bfloat16 [8, 1024, 8192], P('task', None, 'col'), may hold values from -0.29882812 to 0.29882812
- lengths: int32 [8, 4], P('task'), may hold values from 1 to 512, 1024 in all within a row
- task_weights: bfloat16 [8, 8192, 2048], P('task', 'col'), may hold values from -6 to 6
Outputs:
- fisher: float32 [8, 8192, 2048], P('task', 'col')
- merged: bfloat16 [8192, 2048], P('col')
The draws below stay inside these ranges and needn't reach their ends.
Inputs may be any that keep to these rules, and one draw needn't show every extreme that they name: `queries`: queries of every head for the tokens of each task. `key_values`: keys and values of every head for the tokens of each task.
All inputs are finite; a program needn't handle non-finite values.
Results may differ from the reference program's by a relative error of at most 0.02.
Values may be sent and summed in bfloat16 or wider, within the bound.
A program may use at most 64 MiB of HBM per device.

```python
import math
import jax
import jax.numpy as jnp
import numpy as np
from jax import lax

D = 8192
QH = 64
KVH = 8
HD = 128
TOK = 1024
NSEQ = 4
MAXLEN = 512
KVC = 2048
TASKS = 8
N_COL = 32


def shared_fields(key):
    base = jax.random.fold_in(key, 7)
    first, second = jax.random.split(base, 2)
    key_values = jax.random.normal(first, (TASKS, TOK, KVH, 2, HD), jnp.float32)
    key_values = jnp.clip(key_values, -6.0, 6.0)
    queries = jax.random.normal(second, (TASKS, TOK, KVH, QH // KVH, HD), jnp.float32)
    queries = jnp.clip(queries, -6.0, 6.0)
    return (queries.reshape(TASKS, TOK, QH * HD), key_values.reshape(TASKS, TOK, KVH * 2 * HD))


def draw_queries(key, part):
    return shared_fields(key)[0].astype(jnp.bfloat16)


def draw_key_values(key, part):
    return shared_fields(key)[1].astype(jnp.bfloat16)


def levels(key, shape, shards, low, largest):
    def one(axis_at, blocks):
        draws = jax.random.uniform(jax.random.fold_in(jax.random.fold_in(key, 6), axis_at), (blocks,), jnp.float32, low / len(shards), largest / len(shards))
        return jnp.repeat(jnp.exp(draws), shape[axis_at] // blocks).reshape((-1,) + (1,) * (len(shape) - axis_at - 1))

    level = one(*shards[0])
    for cut in shards[1:]:
        level = level * one(*cut)
    return level


def length_profile(amount, total, most, lean):
    portions = [(1 << 20) // math.isqrt(grade ** lean) + 1 for grade in range(2, amount + 1)]
    surplus, holding = total - most - (amount - 1), [1] * (amount - 1)
    while surplus > 0:
        movable = [i for i in range(amount - 1) if holding[i] < most]
        whole, left = sum([portions[i] for i in movable]), surplus
        for i in movable:
            more = min(most - holding[i], max(1, left * portions[i] // whole), surplus)
            holding[i] = holding[i] + more
            surplus = surplus - more
    return np.array([most] + holding)


def uneven(key, amount, total, reach, skew):
    if amount == 2:
        one = jax.random.randint(key, (), max(1, total - reach), min(reach, total - 1) + 1)
        return jnp.stack([one, total - one])
    sizes = jnp.asarray(length_profile(amount, total, reach, skew), jnp.int32)
    twos = (amount - 1) // 2
    donor, sink = sizes[1:1 + 2 * twos:2], sizes[2:2 + 2 * twos:2]
    margin = jnp.minimum(donor - 1, reach - sink)
    shifted = jax.random.randint(jax.random.fold_in(key, 1), (twos,), 0, 1 << 20) % (margin + 1)
    sizes = sizes.at[1:1 + 2 * twos:2].set(donor - shifted).at[2:2 + 2 * twos:2].set(sink + shifted)
    return sizes[jax.random.permutation(jax.random.fold_in(key, 2), amount)]


def normal_values(own_key, extent, width, limit, cuts=(), held_as=jnp.bfloat16):
    gain = levels(own_key, extent, cuts, -0.22, 0.18) if cuts else 1.0
    array = jax.random.normal(own_key, extent, jnp.float32) * width * gain
    return jnp.minimum(jnp.maximum(array, -limit), limit).astype(held_as)


def setup_inputs(seed: int = 0) -> dict:
    streams_of = jax.random.split(jax.random.key(seed), 7)
    return {
        "layer_inputs": normal_values(streams_of[0], (TASKS, TOK, D), 1.0, 6.0, ((0, 8), (2, 32))),
        "queries": draw_queries(jax.random.fold_in(streams_of[6], 71), 0),
        "key_values": draw_key_values(jax.random.fold_in(streams_of[6], 71), 0),
        "out_grads": normal_values(streams_of[3], (TASKS, TOK, QH * HD), 0.05, 0.29882812, ((0, 8), (2, 32))),
        "lengths": jax.vmap(lambda own: uneven(own, NSEQ, TOK, MAXLEN, 2))(jax.random.split(streams_of[4], TASKS)).reshape((TASKS, NSEQ)).astype(jnp.int32),
        "task_weights": normal_values(streams_of[5], (TASKS, D, KVC), 1.0, 6.0, ((0, 8), (1, 32))),
    }


EPS = 1e-6
NEGATIVE = -1e30


def layout(lengths, count):
    lengths = lengths.astype(jnp.int32)
    ending = jnp.cumsum(lengths).astype(jnp.int32)
    starts = (ending - lengths).astype(jnp.int32)
    places = jnp.arange(count, dtype=jnp.int32)
    owner = jnp.sum((places[:, None] >= ending[None, :]).astype(jnp.int32), axis=1).astype(jnp.int32)
    allowed = (owner[:, None] == owner[None, :]) & (places[:, None] >= places[None, :])
    return owner, starts, allowed


def head_grads(head_query, head_keys, head_values, head_cotangent, allowed):
    factor = HD ** -0.5
    scores = jnp.dot(head_query, head_keys.T, preferred_element_type=jnp.float32) * factor
    scores = jnp.where(allowed, scores, NEGATIVE)
    highest = jnp.max(scores, axis=1, keepdims=True)
    summed = jnp.sum(jnp.exp(scores - highest), axis=1, keepdims=True)
    chances = jnp.where(allowed, jnp.exp(scores - highest - jnp.log(summed)), jnp.zeros_like(scores))
    slopes = jnp.dot(head_cotangent, head_values.T, preferred_element_type=jnp.float32)
    offsets = jnp.sum(chances * slopes, axis=1, keepdims=True)
    score_grads = (chances * (slopes - offsets)).astype(jnp.bfloat16)
    value_grads = jnp.dot(chances.astype(jnp.bfloat16).T, head_cotangent, preferred_element_type=jnp.float32)
    key_grads = jnp.dot(score_grads.T, head_query, preferred_element_type=jnp.float32) * factor
    return jnp.concatenate([key_grads, value_grads], axis=1)


def seq_fisher(inputs, grads_all, owner, starts, number_seqs):
    window = inputs.shape[0] // 2
    last_start = inputs.shape[0] - window

    def one_seq(running, number):
        opening = jnp.clip(starts[number], 0, last_start).astype(jnp.int32)
        rows_in = lax.dynamic_slice_in_dim(inputs, opening, window, 0)
        rows_grad = lax.dynamic_slice_in_dim(grads_all, opening, window, 0)
        inside = lax.dynamic_slice_in_dim(owner, opening, window, 0) == number
        rows_grad = jnp.where(inside[:, None], rows_grad, jnp.zeros_like(rows_grad))
        gradient = jnp.dot(rows_in.T, rows_grad, preferred_element_type=jnp.float32)
        return running + gradient * gradient, None

    start_value = jnp.zeros((inputs.shape[1], grads_all.shape[1]), jnp.float32)
    running, unused = lax.scan(one_seq, start_value, jnp.arange(number_seqs, dtype=jnp.int32))
    return running


def task_part(fields):
    inputs, queries, key_values, cotangents, lengths = fields
    count = inputs.shape[0]
    owner, starts, allowed = layout(lengths, count)
    group_heads = QH // KVH
    run_heads = QH // N_COL

    def kv_block(kv_number):
        block = lax.dynamic_slice_in_dim(key_values, kv_number * 2 * HD, 2 * HD, 1)
        head_keys = block[:, :HD]
        head_values = block[:, HD:]
        summed = jnp.zeros((count, 2 * HD), jnp.float32)
        for run_number in range(group_heads // run_heads):
            partial_sum = jnp.zeros((count, 2 * HD), jnp.float32)
            for member in range(run_heads):
                query_number = kv_number * group_heads + run_number * run_heads + member
                head_query = lax.dynamic_slice_in_dim(queries, query_number * HD, HD, 1)
                head_cotangent = lax.dynamic_slice_in_dim(cotangents, query_number * HD, HD, 1)
                partial_sum = partial_sum + head_grads(head_query, head_keys, head_values, head_cotangent, allowed)
            rounded = lax.optimization_barrier(partial_sum.astype(jnp.bfloat16))
            summed = summed + rounded.astype(jnp.float32)
        return summed.astype(jnp.bfloat16)

    blocks = lax.map(kv_block, jnp.arange(KVH, dtype=jnp.int32))
    grads_all = jnp.transpose(blocks, (1, 0, 2)).reshape(count, KVH * 2 * HD)
    return seq_fisher(inputs, grads_all, owner, starts, lengths.shape[0])


def reference(layer_inputs, queries, key_values, out_grads, lengths, task_weights):
    fisher = lax.map(task_part, (layer_inputs, queries, key_values, out_grads, lengths))
    weighted = jnp.sum(fisher * task_weights.astype(jnp.float32), axis=0)
    divisor = jnp.sum(fisher, axis=0) + EPS
    return fisher, (weighted / divisor).astype(jnp.bfloat16)
```

```python
import functools

import jax
import jax.numpy as jnp
from jax import lax
from jax.experimental import pallas as pl
from jax.experimental.pallas import tpu as pltpu
from jax.sharding import PartitionSpec as P

MESH = pl.DeviceIdType.MESH
F32, BF16 = jnp.float32, jnp.bfloat16
KVH = 8
HD = 128
PAIR = 2 * HD
TOK = 1024
BLK = 256
CUT = 96
REST = BLK - CUT
EPS = 1e-06
NEGATIVE = -1e30


class Where:
    def __init__(self):
        self.task, self.col = lax.axis_index("task"), lax.axis_index("col")
        self.y, self.core = self.task // 2, self.task % 2
        self.z, self.x = self.col // 4, self.col % 4

    def along_x(self, by):
        return (self.task, self.z * 4 + (self.x + by + 4) % 4)

    def along_z(self, by):
        return (self.task, ((self.z + by + 8) % 8) * 4 + self.x)

    def along_y(self, by):
        return (((self.y + by) % 4) * 2 + self.core, self.col)

    def other_core(self):
        return (self.y * 2 + 1 - self.core, self.col)


def meet(devices):
    barrier = pltpu.get_barrier_semaphore()
    for device in devices:
        pl.semaphore_signal(barrier, inc=1, device_id=device, device_id_type=MESH)
    pl.semaphore_wait(barrier, len(devices))


class Sender:
    def __init__(self, send_sems, recv_sems):
        self.send_sems, self.recv_sems, self.copies = send_sems, recv_sems, []

    def start(self, src, dst, device):
        at = len(self.copies)
        copy = pltpu.make_async_remote_copy(
            src_ref=src,
            dst_ref=dst,
            send_sem=self.send_sems.at[at],
            recv_sem=self.recv_sems.at[at],
            device_id=device,
            device_id_type=MESH,
        )
        copy.start()
        self.copies.append(copy)
        return copy

    def finish(self):
        for copy in self.copies:
            copy.wait_send()


def bounds(lengths_ref):
    ends, end = [], 0
    for s in range(4):
        end = end + lengths_ref[0, s]
        ends.append(end)
    return ends


def dot_nt(a, b):
    return lax.dot_general(a, b, (((1,), (1,)), ((), ())), preferred_element_type=F32)


def grads_kernel(
    kv_ref, q_ref, og_ref, len_ref, out_ref, kv, score, slope, acc, send_sems, recv_sems, own_sem
):
    at = Where()
    send = Sender(send_sems, recv_sems)
    meet([at.along_x(1), at.along_x(-1)] + [at.along_z(k) for k in range(1, 8)])

    def rows(z, x):
        return pl.ds(pl.multiple_of(z * 128 + x * 32, 32), 32)

    def half(z, x, part):
        return pl.ds(pl.multiple_of(z * 128 + x * 32 + part * 16, 16), 16)

    def head(h):
        return pl.ds(pl.multiple_of(h * PAIR, PAIR), PAIR)

    own = pltpu.make_async_copy(kv_ref.at[:, head(at.z)], kv.at[rows(at.z, at.x)], own_sem)
    own.start()
    steps = (1, 7, 2, 6, 3, 5, 4)
    arrive = {}
    for k in steps:
        arrive[k] = send.start(
            kv_ref.at[:, head((at.z + k) % 8)], kv.at[rows(at.z, at.x)], at.along_z(k)
        )
    own.wait()
    first, second = [], []

    def spread(z):
        block = kv.at[rows(z, at.x)]
        first.append((z, send.start(block, block, at.along_x(1)), send.start(block, block, at.along_x(-1))))

    def pass_on():
        z, up, down = first.pop(0)
        up.wait_recv()
        block = kv.at[half(z, (at.x + 3) % 4, 0)]
        second.append(send.start(block, block, at.along_x(1)))
        down.wait_recv()
        block = kv.at[half(z, (at.x + 1) % 4, 1)]
        second.append(send.start(block, block, at.along_x(-1)))

    spread(at.z)
    for n, k in enumerate(steps):
        arrive[k].wait_recv()
        spread((at.z + 8 - k) % 8)
        if n >= 1:
            pass_on()
    while first:
        pass_on()
    for copy in second:
        copy.wait_recv()

    factor = HD**-0.5
    ends = bounds(len_ref)
    blocks = TOK // BLK
    for i in reversed(range(blocks)):
        queries = pl.ds(i * BLK, BLK)
        low = max(0, i - 2)
        token = i * BLK + lax.broadcasted_iota(jnp.int32, (1, BLK), 1)
        opening = jnp.zeros_like(token)
        for s in range(3):
            opening = jnp.where(token >= ends[s], ends[s], opening)
        for m in range(2):
            lanes = pl.ds(m * HD, HD)
            query = q_ref[queries, lanes]
            cot = og_ref[queries, lanes]
            highest = jnp.full((1, BLK), NEGATIVE, F32)
            for j in range(low, i + 1):
                key = kv[pl.ds(j * BLK, BLK), 0:HD]
                place = j * BLK + lax.broadcasted_iota(jnp.int32, (BLK, BLK), 0)
                allowed = place >= opening
                if j == i:
                    allowed = allowed & (place <= token)
                s = jnp.where(allowed, dot_nt(key, query) * factor, NEGATIVE)
                score[j - low] = s
                highest = jnp.maximum(highest, jnp.max(s, axis=0, keepdims=True))
            total = jnp.zeros((1, BLK), F32)
            weighed = jnp.zeros((1, BLK), F32)
            for j in range(low, i + 1):
                e = jnp.exp(score[j - low] - highest)
                score[j - low] = e
                d = dot_nt(kv[pl.ds(j * BLK, BLK), HD:PAIR], cot)
                slope[j - low] = d
                total = total + jnp.sum(e, axis=0, keepdims=True)
                weighed = weighed + jnp.sum(e * d, axis=0, keepdims=True)
            inverse = 1.0 / total
            offset = weighed * inverse
            for j in range(low, i + 1):
                p = score[j - low] * inverse
                ds = (p * (slope[j - low] - offset)).astype(BF16)
                to = pl.ds(j * BLK, BLK)
                dk = jnp.dot(ds, query, preferred_element_type=F32)
                dv = jnp.dot(p.astype(BF16), cot, preferred_element_type=F32)
                if m == 0 and i == min(blocks - 1, j + 2):
                    acc[to, 0:HD] = dk
                    acc[to, HD:PAIR] = dv
                else:
                    acc[to, 0:HD] += dk
                    acc[to, HD:PAIR] += dv
        done = pl.ds(i * BLK, BLK)
        out_ref[done, 0:HD] = (acc[done, 0:HD] * factor).astype(BF16)
        out_ref[done, HD:PAIR] = acc[done, HD:PAIR].astype(BF16)
    send.finish()


def merge_kernel(
    p_ref,
    x_ref,
    w_ref,
    len_ref,
    fisher_out,
    merged_out,
    xm,
    g,
    half_in,
    half_out,
    fb,
    ps,
    pr,
    ys,
    yr,
    mb,
    send_sems,
    recv_sems,
    out_sems,
):
    at = Where()
    send = Sender(send_sems, recv_sems)
    x, z, y, core = at.x, at.z, at.y, at.core
    meet(
        [at.along_x(1), at.along_x(-1), at.along_z(1), at.along_z(-1), at.other_core()]
        + [at.along_y(k) for k in (1, 2, 3)]
    )

    def quarter(by, part):
        return p_ref.at[
            pl.ds(pl.multiple_of(((x + by + 4) % 4) * BLK, BLK), BLK), part * HD : part * HD + HD
        ]

    far_k = send.start(quarter(2, 0), half_in.at[0], at.along_x(1))
    far_v = send.start(quarter(2, 1), half_in.at[1], at.along_x(-1))
    near_v = send.start(quarter(1, 1), half_in.at[2], at.along_x(1))
    near_k = send.start(quarter(-1, 0), half_in.at[3], at.along_x(-1))

    ends = bounds(len_ref)
    starts = [0] + ends[:3]
    for hf in range(2):
        o = 2 * BLK * hf
        rows = jnp.concatenate(
            [
                x_ref[o : o + CUT],
                x_ref[o + BLK : o + BLK + CUT],
                x_ref[o + CUT : o + BLK],
                x_ref[o + BLK + CUT : o + 2 * BLK],
            ],
            axis=0,
        )
        turned = rows.T
        pos = lax.broadcasted_iota(jnp.int32, (1, 2 * BLK), 1)
        late = pos - 2 * CUT
        token = o + jnp.where(
            pos < 2 * CUT,
            pos + jnp.where(pos >= CUT, BLK - CUT, 0),
            late + CUT + jnp.where(late >= REST, BLK - REST, 0),
        )
        for n in range(3):
            s = hf + n
            inside = jnp.where((token >= starts[s]) & (token < ends[s]), 1.0, 0.0).astype(BF16)
            masked = turned * inside
            for rb in range(2):
                xm[rb, hf, n * HD : (n + 1) * HD, :] = masked[rb * HD : (rb + 1) * HD]

    far_k.wait_recv()
    half_out[0] = (quarter(1, 0)[...].astype(F32) + half_in[0].astype(F32)).astype(BF16)
    sum_k = send.start(half_out.at[0], half_in.at[4], at.along_x(1))
    far_v.wait_recv()
    half_out[1] = (quarter(-1, 1)[...].astype(F32) + half_in[1].astype(F32)).astype(BF16)
    sum_v = send.start(half_out.at[1], half_in.at[5], at.along_x(-1))

    def cut_rows(q):
        return (q // 2, pl.ds(pl.multiple_of(CUT * (q % 2), CUT), CUT))

    def rest_rows(q):
        return (q // 2, pl.ds(pl.multiple_of(2 * CUT + REST * (q % 2), 32), REST))

    def settle(part, near, through):
        own = quarter(0, part)[...].astype(F32) + half_in[near].astype(F32) + half_in[through].astype(F32)
        own = own.astype(BF16)
        lanes = slice(part * HD, part * HD + HD)
        hf, r = cut_rows(x)
        g[z, hf, r, lanes] = own[:CUT]
        hf, r = rest_rows(x)
        g[z, hf, r, lanes] = own[CUT:]

    near_k.wait_recv()
    sum_k.wait_recv()
    settle(0, 3, 4)
    near_v.wait_recv()
    sum_v.wait_recv()
    settle(1, 2, 5)

    def ring_piece(h, place, base, size, part):
        q = (x + place) % 4
        unit = size // 2
        length = size if part is None else unit
        skip = 0 if part is None else part * unit
        start = pl.multiple_of(base + size * (q % 2) + skip, 16)
        return g.at[h, q // 2, pl.ds(start, length)]

    class AroundX:
        def __init__(self, h, base, size):
            self.h, self.base, self.size = h, base, size
            own = ring_piece(h, 0, base, size, None)
            self.up = send.start(own, own, at.along_x(1))
            self.down = send.start(own, own, at.along_x(-1))

        def pass_on(self):
            self.up.wait_recv()
            piece = ring_piece(self.h, 3, self.base, self.size, 0)
            self.up2 = send.start(piece, piece, at.along_x(1))
            self.down.wait_recv()
            piece = ring_piece(self.h, 1, self.base, self.size, 1)
            self.down2 = send.start(piece, piece, at.along_x(-1))

        def end(self):
            self.up2.wait_recv()
            self.down2.wait_recv()

    def head(k):
        return (z + k + 8) % 8

    def send_rest(h, way):
        hf, r = rest_rows(x)
        piece = g.at[h, hf, r]
        return send.start(piece, piece, at.along_z(way))

    def send_cut(h, hf, way):
        piece = g.at[h, hf, 0 : 2 * CUT]
        return send.start(piece, piece, at.along_z(way))

    outs = []

    def columns(h):
        return pl.ds(pl.multiple_of(h * PAIR, PAIR), PAIR)

    def fisher_rows(slot, h, rb):
        a = jnp.dot(xm[rb, 0], g[h, 0], preferred_element_type=F32)
        b = jnp.dot(xm[rb, 1], g[h, 1], preferred_element_type=F32)
        g0, g3 = a[:HD], b[2 * HD :]
        g1, g2 = a[HD : 2 * HD] + b[:HD], a[2 * HD :] + b[HD : 2 * HD]
        f = g0 * g0 + g1 * g1 + g2 * g2 + g3 * g3
        fb[slot, pl.ds(pl.multiple_of(rb * HD, HD), HD), :] = f
        return f

    def weights(h, rb):
        return w_ref[pl.ds(pl.multiple_of(rb * HD, HD), HD), columns(h)].astype(F32)

    pair, over_y, merged_y, merged_core = {}, {}, {}, {}
    heads = [0, -1, 1, -2, 2, -3, 3, 4]

    def compute_other(slot):
        h = head(heads[slot])
        rb = 1 - core
        f = fisher_rows(slot, h, rb)
        ps[slot, 0] = (f * weights(h, rb)).astype(BF16)
        ps[slot, 1] = f.astype(BF16)
        pair[slot] = send.start(ps.at[slot], pr.at[slot], at.other_core())

    def compute_own(slot):
        h = head(heads[slot])
        fisher_rows(slot, h, core)
        copy = pltpu.make_async_copy(fb.at[slot], fisher_out.at[:, columns(h)], out_sems.at[slot])
        copy.start()
        outs.append(copy)

    def sum_pair(slot):
        h = head(heads[slot])
        pair[slot].wait_recv()
        f = fb[slot, pl.ds(pl.multiple_of(core * HD, HD), HD), :]
        ys[slot, 0] = (f * weights(h, core) + pr[slot, 0].astype(F32)).astype(BF16)
        ys[slot, 1] = (f + pr[slot, 1].astype(F32)).astype(BF16)
        over_y[slot] = []
        for k in (2, 1, 3):
            rows = pl.ds(pl.multiple_of(((y + k) % 4) * 32, 32), 32)
            over_y[slot].append(send.start(ys.at[slot, :, rows], yr.at[slot, k - 1], at.along_y(k)))

    def divide(slot):
        h = head(heads[slot])
        for copy in over_y[slot]:
            copy.wait_recv()
        rows = pl.ds(pl.multiple_of(y * 32, 32), 32)
        sums = ys[slot, :, rows, :].astype(F32)
        for k in range(3):
            sums = sums + yr[slot, k].astype(F32)
        to = pl.ds(pl.multiple_of(core * HD + y * 32, 32), 32)
        mb[h, to, :] = (sums[0] / (sums[1] + EPS)).astype(BF16)
        piece = mb.at[h, to]
        merged_y[slot] = [send.start(piece, piece, at.along_y(k)) for k in (2, 1, 3)]

    def share(slot):
        h = head(heads[slot])
        for copy in merged_y[slot]:
            copy.wait_recv()
        piece = mb.at[h, pl.ds(pl.multiple_of(core * HD, HD), HD)]
        merged_core[slot] = send.start(piece, piece, at.other_core())

    def close(slot):
        h = head(heads[slot])
        merged_core[slot].wait_recv()
        copy = pltpu.make_async_copy(mb.at[h], merged_out.at[:, columns(h)], out_sems.at[8 + slot])
        copy.start()
        outs.append(copy)

    stages = (sum_pair, divide, share, close)
    progress = {s: 0 for s in range(8)}

    def advance(upto):
        for slot in range(upto):
            if progress[slot] < len(stages):
                stages[progress[slot]](slot)
                progress[slot] += 1

    rest_up = send_rest(z, 1)
    rest_down = send_rest(z, -1)
    cut_ring = AroundX(z, 0, CUT)
    rings = [AroundX(z, 2 * CUT, REST)]
    cut_ring.pass_on()
    cut_ring.end()
    up0, down0 = send_cut(z, 0, 1), send_cut(z, 0, -1)
    up1, down1 = send_cut(z, 1, 1), send_cut(z, 1, -1)
    rings[0].pass_on()
    rings[0].end()
    ready = [0]

    for k in range(1, 5):
        above, below = head(-k), head(k)
        rings = []
        if k < 4:
            rest_up.wait_recv()
            rings.append(AroundX(above, 2 * CUT, REST))
            if k < 3:
                rest_up, up_old = send_rest(above, 1), rest_up
        rest_down.wait_recv()
        rings.append(AroundX(below, 2 * CUT, REST))
        if k < 4:
            rest_down = send_rest(below, -1)
        if k == 3:
            rest_up = None
        work = []
        for slot in ready:
            work += [functools.partial(compute_other, slot), functools.partial(compute_own, slot)]
        done = ready[-1] + 1

        def next_work():
            if work:
                work.pop(0)()

        next_work()
        up0.wait_recv()
        if k < 4:
            up0 = send_cut(above, 0, 1)
            down0.wait_recv()
            if k < 3:
                down0 = send_cut(below, 0, -1)
        next_work()
        for ring in rings:
            ring.pass_on()
        next_work()
        if k < 4:
            up1.wait_recv()
            if k < 3:
                up1 = send_cut(above, 1, 1)
        down1.wait_recv()
        if k < 4:
            down1 = send_cut(below, 1, -1)
        next_work()
        for ring in rings:
            ring.end()
        advance(done)
        ready = [2 * k - 1, 2 * k] if k < 4 else [7]

    compute_other(7)
    compute_own(7)
    while any(progress[s] < len(stages) for s in range(8)):
        advance(8)
    send.finish()
    for copy in outs:
        copy.wait()


def vmem():
    return pl.BlockSpec(memory_space=pltpu.VMEM)


def body(layer_inputs, queries, key_values, out_grads, lengths, task_weights):
    smem = pl.BlockSpec(memory_space=pltpu.SMEM)
    partial = pl.pallas_call(
        grads_kernel,
        out_shape=jax.ShapeDtypeStruct((TOK, PAIR), BF16),
        in_specs=[vmem(), vmem(), vmem(), smem],
        out_specs=vmem(),
        scratch_shapes=[
            pltpu.VMEM((TOK, PAIR), BF16),
            pltpu.VMEM((3, BLK, BLK), F32),
            pltpu.VMEM((3, BLK, BLK), F32),
            pltpu.VMEM((TOK, PAIR), F32),
            pltpu.SemaphoreType.DMA((39,)),
            pltpu.SemaphoreType.DMA((39,)),
            pltpu.SemaphoreType.DMA,
        ],
        compiler_params=pltpu.CompilerParams(collective_id=0, has_side_effects=True),
        name="grads",
    )(key_values[0], queries[0], out_grads[0], lengths)
    fisher, merged = pl.pallas_call(
        merge_kernel,
        out_shape=(
            jax.ShapeDtypeStruct((BLK, KVH * PAIR), F32),
            jax.ShapeDtypeStruct((BLK, KVH * PAIR), BF16),
        ),
        in_specs=[vmem(), vmem(), vmem(), smem],
        out_specs=(pl.BlockSpec(memory_space=pl.ANY), pl.BlockSpec(memory_space=pl.ANY)),
        scratch_shapes=[
            pltpu.VMEM((2, 2, 3 * HD, 2 * BLK), BF16),
            pltpu.VMEM((KVH, 2, 2 * BLK, PAIR), BF16),
            pltpu.VMEM((6, BLK, HD), BF16),
            pltpu.VMEM((2, BLK, HD), BF16),
            pltpu.VMEM((8, BLK, PAIR), F32),
            pltpu.VMEM((8, 2, HD, PAIR), BF16),
            pltpu.VMEM((8, 2, HD, PAIR), BF16),
            pltpu.VMEM((8, 2, HD, PAIR), BF16),
            pltpu.VMEM((8, 3, 2, 32, PAIR), BF16),
            pltpu.VMEM((KVH, BLK, PAIR), BF16),
            pltpu.SemaphoreType.DMA((132,)),
            pltpu.SemaphoreType.DMA((132,)),
            pltpu.SemaphoreType.DMA((16,)),
        ],
        compiler_params=pltpu.CompilerParams(collective_id=1, has_side_effects=True),
        name="merge",
    )(partial, layer_inputs[0], task_weights[0], lengths)
    return fisher[None], merged


def solution(mesh):
    placed = (
        P("task", None, "col"),
        P("task", None, "col"),
        P("task", "col", None),
        P("task", None, "col"),
        P("task", None),
        P("task", "col", None),
    )
    return jax.shard_map(
        body,
        mesh=mesh,
        in_specs=placed,
        out_specs=(P("task", "col", None), P("col", None)),
        check_vma=False,
    )
```

```python
import functools

import jax
import jax.numpy as jnp
from jax import lax
from jax.experimental import pallas as pl
from jax.experimental.pallas import tpu as pltpu
from jax.sharding import PartitionSpec as P

MESH = pl.DeviceIdType.MESH
F32, BF16 = jnp.float32, jnp.bfloat16
KVH = 8
HD = 128
PAIR = 2 * HD
TOK = 1024
BLK = 256
CUT = 96
REST = BLK - CUT
EPS = 1e-06
NEGATIVE = -1e30
SEMS = 164


class Where:
    def __init__(self):
        self.task, self.col = lax.axis_index("task"), lax.axis_index("col")
        self.y, self.core = self.task // 2, self.task % 2
        self.z, self.x = self.col // 4, self.col % 4

    def along_x(self, by):
        return (self.task, self.z * 4 + (self.x + by + 4) % 4)

    def along_z(self, by):
        return (self.task, ((self.z + by + 8) % 8) * 4 + self.x)

    def along_y(self, by, across=False):
        core = 1 - self.core if across else self.core
        return (((self.y + by) % 4) * 2 + core, self.col)

    def other_core(self):
        return (self.y * 2 + 1 - self.core, self.col)


def meet(devices):
    barrier = pltpu.get_barrier_semaphore()
    for device in devices:
        pl.semaphore_signal(barrier, inc=1, device_id=device, device_id_type=MESH)
    pl.semaphore_wait(barrier, len(devices))


class Sender:
    def __init__(self, send_sems, recv_sems):
        self.send_sems, self.recv_sems, self.copies = send_sems, recv_sems, []

    def start(self, src, dst, device):
        at = len(self.copies)
        copy = pltpu.make_async_remote_copy(
            src_ref=src,
            dst_ref=dst,
            send_sem=self.send_sems.at[at],
            recv_sem=self.recv_sems.at[at],
            device_id=device,
            device_id_type=MESH,
        )
        copy.start()
        self.copies.append(copy)
        return copy

    def finish(self):
        for copy in self.copies:
            copy.wait_send()


def bounds(lengths_ref):
    ends, end = [], 0
    for s in range(4):
        end = end + lengths_ref[0, s]
        ends.append(end)
    return ends


def dot_nt(a, b):
    return lax.dot_general(a, b, (((1,), (1,)), ((), ())), preferred_element_type=F32)


def step_kernel(
    kv_hbm,
    q_hbm,
    og_hbm,
    x_hbm,
    w_hbm,
    len_ref,
    fisher_out,
    merged_out,
    kv_ref,
    q_ref,
    og_ref,
    x_ref,
    w_ref,
    kv,
    score,
    slope,
    acc,
    p_ref,
    rs_in,
    xm,
    g,
    fb,
    ps,
    pr,
    ys,
    yr,
    mb,
    send_sems,
    recv_sems,
    block_send,
    block_recv,
    local_sems,
):
    at = Where()
    send = Sender(send_sems, recv_sems)
    x, z, y, core = at.x, at.z, at.y, at.core

    loads = []
    for n, (src, dst) in enumerate(
        ((kv_hbm, kv_ref), (q_hbm, q_ref), (og_hbm, og_ref), (x_hbm, x_ref), (w_hbm, w_ref))
    ):
        copy = pltpu.make_async_copy(src, dst, local_sems.at[n])
        copy.start()
        loads.append(copy)
    meet(
        [at.along_z(k) for k in (4, 3, 5, 2, 6, 1, 7)]
        + [at.along_y(k) for k in (2, 1, 3)]
        + [at.along_y(k, True) for k in (2, 1, 3)]
        + [at.along_x(1), at.along_x(-1), at.other_core()]
    )

    def rows(z, x):
        return pl.ds(pl.multiple_of(z * 128 + x * 32, 32), 32)

    def half(z, x, part):
        return pl.ds(pl.multiple_of(z * 128 + x * 32 + part * 16, 16), 16)

    def columns(h):
        return pl.ds(pl.multiple_of(h * PAIR, PAIR), PAIR)

    loads[0].wait()
    steps = (1, 7, 2, 6, 3, 5, 4)
    arrive = {}
    for k in (4, 3, 5, 2, 6, 1, 7):
        arrive[k] = send.start(
            kv_ref.at[:, columns((z + k) % 8)], kv.at[rows(z, x)], at.along_z(k)
        )
    own = pltpu.make_async_copy(kv_ref.at[:, columns(z)], kv.at[rows(z, x)], local_sems.at[5])
    own.start()
    own.wait()
    first, second = [], []

    def spread(z):
        block = kv.at[rows(z, x)]
        first.append((z, send.start(block, block, at.along_x(1)), send.start(block, block, at.along_x(-1))))

    spread(z)
    for k in steps:
        arrive[k].wait_recv()
        spread((z + 8 - k) % 8)
    for z_of, up, down in first:
        up.wait_recv()
        block = kv.at[half(z_of, (x + 3) % 4, 0)]
        second.append(send.start(block, block, at.along_x(1)))
        down.wait_recv()
        block = kv.at[half(z_of, (x + 1) % 4, 1)]
        second.append(send.start(block, block, at.along_x(-1)))
    for copy in loads[1:3]:
        copy.wait()
    for copy in second:
        copy.wait_recv()

    factor = HD**-0.5
    ends = bounds(len_ref)
    blocks = TOK // BLK

    def block_copy(j):
        by = (j - x + 4) % 4
        done = pl.ds(j * BLK, BLK)
        return pltpu.make_async_remote_copy(
            src_ref=p_ref.at[done],
            dst_ref=rs_in.at[by - 1],
            send_sem=block_send.at[j],
            recv_sem=block_recv.at[by - 1],
            device_id=(at.task, z * 4 + j),
            device_id_type=MESH,
        )

    for i in reversed(range(blocks)):
        queries = pl.ds(i * BLK, BLK)
        low = max(0, i - 2)
        token = i * BLK + lax.broadcasted_iota(jnp.int32, (1, BLK), 1)
        opening = jnp.zeros_like(token)
        for s in range(3):
            opening = jnp.where(token >= ends[s], ends[s], opening)
        for m in range(2):
            lanes = pl.ds(m * HD, HD)
            query = q_ref[queries, lanes]
            cot = og_ref[queries, lanes]
            highest = jnp.full((1, BLK), NEGATIVE, F32)
            for j in range(low, i + 1):
                key = kv[pl.ds(j * BLK, BLK), 0:HD]
                place = j * BLK + lax.broadcasted_iota(jnp.int32, (BLK, BLK), 0)
                allowed = place >= opening
                if j == i:
                    allowed = allowed & (place <= token)
                s = jnp.where(allowed, dot_nt(key, query) * factor, NEGATIVE)
                score[j - low] = s
                highest = jnp.maximum(highest, jnp.max(s, axis=0, keepdims=True))
            total = jnp.zeros((1, BLK), F32)
            weighed = jnp.zeros((1, BLK), F32)
            for j in range(low, i + 1):
                e = jnp.exp(score[j - low] - highest)
                score[j - low] = e
                d = dot_nt(kv[pl.ds(j * BLK, BLK), HD:PAIR], cot)
                slope[j - low] = d
                total = total + jnp.sum(e, axis=0, keepdims=True)
                weighed = weighed + jnp.sum(e * d, axis=0, keepdims=True)
            inverse = 1.0 / total
            offset = weighed * inverse
            for j in range(low, i + 1):
                p = score[j - low] * inverse
                ds = (p * (slope[j - low] - offset)).astype(BF16)
                to = pl.ds(j * BLK, BLK)
                dk = jnp.dot(ds, query, preferred_element_type=F32)
                dv = jnp.dot(p.astype(BF16), cot, preferred_element_type=F32)
                if m == 0 and i == min(blocks - 1, j + 2):
                    acc[to, 0:HD] = dk
                    acc[to, HD:PAIR] = dv
                else:
                    acc[to, 0:HD] += dk
                    acc[to, HD:PAIR] += dv
        done = pl.ds(i * BLK, BLK)
        p_ref[done, 0:HD] = (acc[done, 0:HD] * factor).astype(BF16)
        p_ref[done, HD:PAIR] = acc[done, HD:PAIR].astype(BF16)

        @pl.when(x != i)
        def _(i=i):
            block_copy(i).start()

    loads[3].wait()
    starts = [0] + ends[:3]
    for hf in range(2):
        o = 2 * BLK * hf
        turned = jnp.concatenate(
            [
                x_ref[o : o + CUT],
                x_ref[o + BLK : o + BLK + CUT],
                x_ref[o + CUT : o + BLK],
                x_ref[o + BLK + CUT : o + 2 * BLK],
            ],
            axis=0,
        ).T
        pos = lax.broadcasted_iota(jnp.int32, (1, 2 * BLK), 1)
        late = pos - 2 * CUT
        token = o + jnp.where(
            pos < 2 * CUT,
            pos + jnp.where(pos >= CUT, BLK - CUT, 0),
            late + CUT + jnp.where(late >= REST, BLK - REST, 0),
        )
        for n in range(3):
            s = hf + n
            inside = jnp.where((token >= starts[s]) & (token < ends[s]), 1.0, 0.0).astype(BF16)
            masked = turned * inside
            for rb in range(2):
                xm[rb, hf, n * HD : (n + 1) * HD, :] = masked[rb * HD : (rb + 1) * HD]
    loads[4].wait()

    def cut_rows(q):
        return (q // 2, pl.ds(pl.multiple_of(CUT * (q % 2), CUT), CUT))

    def rest_rows(q):
        return (q // 2, pl.ds(pl.multiple_of(2 * CUT + REST * (q % 2), 32), REST))

    summed = p_ref[pl.ds(pl.multiple_of(x * BLK, BLK), BLK), :].astype(F32)
    for by in range(3):
        pltpu.make_async_remote_copy(
            src_ref=p_ref.at[0:BLK],
            dst_ref=rs_in.at[by],
            send_sem=block_send.at[0],
            recv_sem=block_recv.at[by],
            device_id=at.along_x(1),
            device_id_type=MESH,
        ).wait_recv()
        summed = summed + rs_in[by].astype(F32)
    summed = summed.astype(BF16)
    hf, r = cut_rows(x)
    g[z, hf, r, :] = summed[:CUT]
    hf, r = rest_rows(x)
    g[z, hf, r, :] = summed[CUT:]

    def ring_piece(h, place, base, size, part):
        q = (x + place) % 4
        unit = size // 2
        length = size if part is None else unit
        skip = 0 if part is None else part * unit
        start = pl.multiple_of(base + size * (q % 2) + skip, 16)
        return g.at[h, q // 2, pl.ds(start, length)]

    class AroundX:
        def __init__(self, h, base, size):
            self.h, self.base, self.size = h, base, size
            own = ring_piece(h, 0, base, size, None)
            self.up = send.start(own, own, at.along_x(1))
            self.down = send.start(own, own, at.along_x(-1))

        def pass_on(self):
            self.up.wait_recv()
            piece = ring_piece(self.h, 3, self.base, self.size, 0)
            self.up2 = send.start(piece, piece, at.along_x(1))
            self.down.wait_recv()
            piece = ring_piece(self.h, 1, self.base, self.size, 1)
            self.down2 = send.start(piece, piece, at.along_x(-1))

        def end(self):
            self.up2.wait_recv()
            self.down2.wait_recv()

    def head(k):
        return (z + k + 8) % 8

    def send_rest(h, way):
        hf, r = rest_rows(x)
        piece = g.at[h, hf, r]
        return send.start(piece, piece, at.along_z(way))

    def send_cut(h, hf, way):
        piece = g.at[h, hf, 0 : 2 * CUT]
        return send.start(piece, piece, at.along_z(way))

    heads = [0, -1, 1, -2, 2, -3, 3, 4]
    outs = []

    def fisher_rows(slot, h, rb):
        a = jnp.dot(xm[rb, 0], g[h, 0], preferred_element_type=F32)
        b = jnp.dot(xm[rb, 1], g[h, 1], preferred_element_type=F32)
        g0, g3 = a[:HD], b[2 * HD :]
        g1, g2 = a[HD : 2 * HD] + b[:HD], a[2 * HD :] + b[HD : 2 * HD]
        f = g0 * g0 + g1 * g1 + g2 * g2 + g3 * g3
        fb[slot, pl.ds(pl.multiple_of(rb * HD, HD), HD), :] = f
        return f

    def weights(h, rb):
        return w_ref[pl.ds(pl.multiple_of(rb * HD, HD), HD), columns(h)].astype(F32)

    pair, over_y, merged_y, merged_core = {}, {}, {}, {}

    def compute_other(slot):
        h = head(heads[slot])
        rb = 1 - core
        f = fisher_rows(slot, h, rb)
        ps[slot, 0] = (f * weights(h, rb)).astype(BF16)
        ps[slot, 1] = f.astype(BF16)
        pair[slot] = send.start(ps.at[slot], pr.at[slot], at.other_core())

    def compute_own(slot):
        h = head(heads[slot])
        fisher_rows(slot, h, core)
        copy = pltpu.make_async_copy(fb.at[slot], fisher_out.at[:, columns(h)], local_sems.at[6 + slot])
        copy.start()
        outs.append(copy)

    def sum_pair(slot):
        h = head(heads[slot])
        pair[slot].wait_recv()
        f = fb[slot, pl.ds(pl.multiple_of(core * HD, HD), HD), :]
        ys[slot, 0] = (f * weights(h, core) + pr[slot, 0].astype(F32)).astype(BF16)
        ys[slot, 1] = (f + pr[slot, 1].astype(F32)).astype(BF16)
        over_y[slot] = []
        for k in (2, 1, 3):
            r = pl.ds(pl.multiple_of(((y + k) % 4) * 32, 32), 32)
            over_y[slot].append(send.start(ys.at[slot, :, r], yr.at[slot, k - 1], at.along_y(k)))

    def divide(slot):
        h = head(heads[slot])
        for copy in over_y[slot]:
            copy.wait_recv()
        r = pl.ds(pl.multiple_of(y * 32, 32), 32)
        sums = ys[slot, :, r, :].astype(F32)
        for k in range(3):
            sums = sums + yr[slot, k].astype(F32)
        to = pl.ds(pl.multiple_of(core * HD + y * 32, 32), 32)
        mb[h, to, :] = (sums[0] / (sums[1] + EPS)).astype(BF16)
        piece = mb.at[h, to]
        merged_y[slot] = [send.start(piece, piece, at.along_y(k)) for k in (2, 1, 3)]
        if slot == 7:
            merged_y[slot] += [send.start(piece, piece, at.along_y(k, True)) for k in (2, 1, 3)]
            merged_y[slot].append(send.start(piece, piece, at.other_core()))

    def share(slot):
        h = head(heads[slot])
        for copy in merged_y[slot]:
            copy.wait_recv()
        if slot < 7:
            piece = mb.at[h, pl.ds(pl.multiple_of(core * HD, HD), HD)]
            merged_core[slot] = send.start(piece, piece, at.other_core())

    def close(slot):
        h = head(heads[slot])
        if slot < 7:
            merged_core[slot].wait_recv()
        copy = pltpu.make_async_copy(mb.at[h], merged_out.at[:, columns(h)], local_sems.at[14 + slot])
        copy.start()
        outs.append(copy)

    stages = (sum_pair, divide, share, close)
    progress = {s: 0 for s in range(8)}

    def advance(upto):
        for slot in range(upto):
            if progress[slot] < len(stages):
                stages[progress[slot]](slot)
                progress[slot] += 1

    rings = {}
    rest = {"up": send_rest(z, 1), "down": send_rest(z, -1)}

    def rest_hop(k):
        if k < 4:
            rest["up"].wait_recv()
            if k < 3:
                rest["up"] = send_rest(head(-k), 1)
        rest["down"].wait_recv()
        if k < 4:
            rest["down"] = send_rest(head(k), -1)

    def around(slot):
        rings[slot] = AroundX(head(heads[slot]), 2 * CUT, REST)

    cut = {}

    def cut_hop(k, hf):
        last_up, last_down = (4, 3) if hf == 0 else (3, 4)
        if k <= last_up:
            cut["up", hf].wait_recv()
            if k < last_up:
                cut["up", hf] = send_cut(head(-k), hf, 1)
        if k <= last_down:
            cut["down", hf].wait_recv()
            if k < last_down:
                cut["down", hf] = send_cut(head(k), hf, -1)

    cut_ring = AroundX(z, 0, CUT)
    around(0)
    cut_ring.pass_on()
    rest_hop(1)
    around(1)
    cut_ring.end()
    for hf in range(2):
        for name, way in (("up", 1), ("down", -1)):
            cut[name, hf] = send_cut(z, hf, way)
    rings[0].pass_on()
    around(2)
    rest_hop(2)
    rings[0].end()
    compute_other(0)
    for j in range(1, 8):
        rings[j].pass_on()
        if j + 2 < 8:
            around(j + 2)
        if j == 1:
            compute_own(0)
        elif j == 2:
            rest_hop(3)
            cut_hop(1, 0)
        elif j == 3:
            cut_hop(1, 1)
            rings[1].end()
            compute_other(1)
            compute_own(1)
            rest_hop(4)
        elif j == 4:
            cut_hop(2, 0)
            rings[2].end()
            compute_other(2)
            compute_own(2)
        elif j == 5:
            cut_hop(2, 1)
            rings[3].end()
            compute_other(3)
            compute_own(3)
        elif j == 6:
            cut_hop(3, 0)
            rings[4].end()
            compute_other(4)
            compute_own(4)
        elif j == 7:
            cut_hop(3, 1)
            rings[5].end()
            compute_other(5)
            compute_own(5)
        advance(max(0, min(j - 2, 8)))
    rings[6].end()
    compute_other(6)
    compute_own(6)
    advance(6)
    cut_hop(4, 0)
    cut_hop(4, 1)
    rings[7].end()
    compute_other(7)
    compute_own(7)
    while any(progress[s] < len(stages) for s in range(8)):
        advance(8)
    send.finish()
    for copy in outs:
        copy.wait()
    for j in range(blocks):

        @pl.when(x != j)
        def _(j=j):
            block_copy(j).wait_send()


def write_kernel(fisher_ref, merged_ref, fisher_out, merged_out):
    fisher_out[...] = fisher_ref[...]
    merged_out[...] = merged_ref[...]


def body(layer_inputs, queries, key_values, out_grads, lengths, task_weights):
    hbm = pl.BlockSpec(memory_space=pl.ANY)
    wide = KVH * PAIR
    results = (
        jax.ShapeDtypeStruct((BLK, wide), F32),
        jax.ShapeDtypeStruct((BLK, wide), BF16),
    )
    fisher, merged = pl.pallas_call(
        step_kernel,
        out_shape=results,
        in_specs=[hbm] * 5 + [pl.BlockSpec(memory_space=pltpu.SMEM)],
        out_specs=(hbm, hbm),
        scratch_shapes=[
            pltpu.VMEM((TOK // 32, wide), BF16),
            pltpu.VMEM((TOK, PAIR), BF16),
            pltpu.VMEM((TOK, PAIR), BF16),
            pltpu.VMEM((TOK, BLK), BF16),
            pltpu.VMEM((BLK, wide), BF16),
            pltpu.VMEM((TOK, PAIR), BF16),
            pltpu.VMEM((3, BLK, BLK), F32),
            pltpu.VMEM((3, BLK, BLK), F32),
            pltpu.VMEM((TOK, PAIR), F32),
            pltpu.VMEM((TOK, PAIR), BF16),
            pltpu.VMEM((3, BLK, PAIR), BF16),
            pltpu.VMEM((2, 2, 3 * HD, 2 * BLK), BF16),
            pltpu.VMEM((KVH, 2, 2 * BLK, PAIR), BF16),
            pltpu.VMEM((8, BLK, PAIR), F32),
            pltpu.VMEM((8, 2, HD, PAIR), BF16),
            pltpu.VMEM((8, 2, HD, PAIR), BF16),
            pltpu.VMEM((8, 2, HD, PAIR), BF16),
            pltpu.VMEM((8, 3, 2, 32, PAIR), BF16),
            pltpu.VMEM((KVH, BLK, PAIR), BF16),
            pltpu.SemaphoreType.DMA((SEMS,)),
            pltpu.SemaphoreType.DMA((SEMS,)),
            pltpu.SemaphoreType.DMA((4,)),
            pltpu.SemaphoreType.DMA((3,)),
            pltpu.SemaphoreType.DMA((22,)),
        ],
        compiler_params=pltpu.CompilerParams(collective_id=0, has_side_effects=True),
        name="step",
    )(key_values[0], queries[0], out_grads[0], layer_inputs[0], task_weights[0], lengths)
    blocks = [
        pl.BlockSpec((BLK // 4, wide), lambda i: (i, 0)),
        pl.BlockSpec((BLK // 4, wide), lambda i: (i, 0)),
    ]
    fisher, merged = pl.pallas_call(
        write_kernel,
        out_shape=results,
        grid=(4,),
        in_specs=blocks,
        out_specs=tuple(blocks),
        name="write",
    )(fisher, merged)
    return fisher[None], merged


def solution(mesh):
    placed = (
        P("task", None, "col"),
        P("task", None, "col"),
        P("task", "col", None),
        P("task", None, "col"),
        P("task", None),
        P("task", "col", None),
    )
    return jax.shard_map(
        body,
        mesh=mesh,
        in_specs=placed,
        out_specs=(P("task", "col", None), P("col", None)),
        check_vma=False,
    )
```

```python
import functools

import jax
import jax.numpy as jnp
from jax import lax
from jax.experimental import pallas as pl
from jax.experimental.pallas import tpu as pltpu
from jax.sharding import PartitionSpec as P

MESH = pl.DeviceIdType.MESH
F32, BF16 = jnp.float32, jnp.bfloat16
KVH = 8
HD = 128
PAIR = 2 * HD
TOK = 1024
BLK = 256
CUT = 96
REST = BLK - CUT
EPS = 1e-06
NEGATIVE = -1e30
TURNS = 24
SEMS = 88


class Where:
    def __init__(self):
        self.task, self.col = lax.axis_index("task"), lax.axis_index("col")
        self.y, self.core = self.task // 2, self.task % 2
        self.z, self.x = self.col // 4, self.col % 4

    def along_x(self, by):
        return (self.task, self.z * 4 + (self.x + by + 4) % 4)

    def along_z(self, by):
        return (self.task, ((self.z + by + 8) % 8) * 4 + self.x)

    def along_y(self, by, across=False):
        core = 1 - self.core if across else self.core
        return (((self.y + by) % 4) * 2 + core, self.col)

    def other_core(self):
        return (self.y * 2 + 1 - self.core, self.col)


def meet(devices):
    barrier = pltpu.get_barrier_semaphore()
    for device in devices:
        pl.semaphore_signal(barrier, inc=1, device_id=device, device_id_type=MESH)
    pl.semaphore_wait(barrier, len(devices))


class Sender:
    def __init__(self, send_sems, recv_sems):
        self.send_sems, self.recv_sems = send_sems, recv_sems
        self.copies, self.used = [], 0

    def fresh(self):
        self.used += 1
        assert self.used <= SEMS
        return self.recv_sems.at[self.used - 1]

    def start(self, src, dst, device, recv_sem=None):
        at = len(self.copies)
        if at >= TURNS:
            self.copies[at - TURNS].wait_send()
        copy = pltpu.make_async_remote_copy(
            src_ref=src,
            dst_ref=dst,
            send_sem=self.send_sems.at[at % TURNS],
            recv_sem=self.fresh() if recv_sem is None else recv_sem,
            device_id=device,
            device_id_type=MESH,
        )
        copy.start()
        self.copies.append(copy)
        return copy

    def arrived(self, ref, recv_sem):
        pltpu.make_async_remote_copy(
            src_ref=ref,
            dst_ref=ref,
            send_sem=self.send_sems.at[0],
            recv_sem=recv_sem,
            device_id=(0, 0),
            device_id_type=MESH,
        ).wait_recv()

    def finish(self):
        for copy in self.copies[-TURNS:]:
            copy.wait_send()


def bounds(lengths_ref):
    ends, end = [], 0
    for s in range(4):
        end = end + lengths_ref[0, s]
        ends.append(end)
    return ends


def dot_nt(a, b):
    return lax.dot_general(a, b, (((1,), (1,)), ((), ())), preferred_element_type=F32)


def step_kernel(
    kv_hbm,
    q_hbm,
    og_hbm,
    x_hbm,
    w_hbm,
    len_ref,
    fisher_out,
    merged_out,
    kv_ref,
    q_ref,
    og_ref,
    x_ref,
    w_ref,
    kv,
    score,
    slope,
    acc,
    p_ref,
    rs_in,
    xm,
    g,
    fb,
    ps,
    pr,
    ys,
    yr,
    mb,
    send_sems,
    recv_sems,
    block_send,
    block_recv,
    local_sems,
):
    at = Where()
    send = Sender(send_sems, recv_sems)
    x, z, y, core = at.x, at.z, at.y, at.core

    loads = []
    for n, (src, dst) in enumerate(
        ((kv_hbm, kv_ref), (q_hbm, q_ref), (og_hbm, og_ref), (x_hbm, x_ref), (w_hbm, w_ref))
    ):
        copy = pltpu.make_async_copy(src, dst, local_sems.at[n])
        copy.start()
        loads.append(copy)
    meet(
        [at.along_z(k) for k in (4, 3, 5, 2, 6, 1, 7)]
        + [at.along_y(k) for k in (2, 1, 3)]
        + [at.along_y(k, True) for k in (2, 1, 3)]
        + [at.along_x(2), at.along_x(1), at.along_x(-1), at.other_core()]
    )

    def rows(z, x):
        return pl.ds(pl.multiple_of(z * 128 + x * 32, 32), 32)

    def columns(h):
        return pl.ds(pl.multiple_of(h * PAIR, PAIR), PAIR)

    loads[0].wait()
    own = pltpu.make_async_copy(kv_ref.at[:, columns(z)], kv.at[rows(z, x)], local_sems.at[5])
    own.start()
    steps = (1, 7, 2, 6, 3, 5, 4)
    spare = {k: send.fresh() for k in steps}
    arrive = {
        k: send.start(kv_ref.at[:, columns((z + k) % 8)], kv.at[rows(z, x)], at.along_z(k), spare[k])
        for k in steps
    }
    spare = list(spare.values())
    spread = []

    def spread_block(z):
        block = kv.at[rows(z, x)]
        for by in (2, 1, -1):
            spare.append(send.fresh())
            spread.append(send.start(block, block, at.along_x(by), spare[-1]))

    own.wait()
    spread_block(z)
    for k in steps:
        arrive[k].wait_recv()
        spread_block((z + 8 - k) % 8)
    for copy in loads[1:3]:
        copy.wait()
    for copy in spread:
        copy.wait_recv()

    factor = HD**-0.5
    ends = bounds(len_ref)
    blocks = TOK // BLK

    def block_copy(j):
        by = (j - x + 4) % 4
        done = pl.ds(j * BLK, BLK)
        return pltpu.make_async_remote_copy(
            src_ref=p_ref.at[done],
            dst_ref=rs_in.at[by - 1],
            send_sem=block_send.at[j],
            recv_sem=block_recv.at[by - 1],
            device_id=(at.task, z * 4 + j),
            device_id_type=MESH,
        )

    for i in reversed(range(blocks)):
        queries = pl.ds(i * BLK, BLK)
        low = max(0, i - 2)
        token = i * BLK + lax.broadcasted_iota(jnp.int32, (1, BLK), 1)
        opening = jnp.zeros_like(token)
        for s in range(3):
            opening = jnp.where(token >= ends[s], ends[s], opening)
        for m in range(2):
            lanes = pl.ds(m * HD, HD)
            query = q_ref[queries, lanes]
            cot = og_ref[queries, lanes]
            highest = jnp.full((1, BLK), NEGATIVE, F32)
            for j in range(low, i + 1):
                key = kv[pl.ds(j * BLK, BLK), 0:HD]
                place = j * BLK + lax.broadcasted_iota(jnp.int32, (BLK, BLK), 0)
                allowed = place >= opening
                if j == i:
                    allowed = allowed & (place <= token)
                s = jnp.where(allowed, dot_nt(key, query) * factor, NEGATIVE)
                score[j - low] = s
                highest = jnp.maximum(highest, jnp.max(s, axis=0, keepdims=True))
            total = jnp.zeros((1, BLK), F32)
            weighed = jnp.zeros((1, BLK), F32)
            for j in range(low, i + 1):
                e = jnp.exp(score[j - low] - highest)
                score[j - low] = e
                d = dot_nt(kv[pl.ds(j * BLK, BLK), HD:PAIR], cot)
                slope[j - low] = d
                total = total + jnp.sum(e, axis=0, keepdims=True)
                weighed = weighed + jnp.sum(e * d, axis=0, keepdims=True)
            inverse = 1.0 / total
            offset = weighed * inverse
            for j in range(low, i + 1):
                p = score[j - low] * inverse
                ds = (p * (slope[j - low] - offset)).astype(BF16)
                to = pl.ds(j * BLK, BLK)
                dk = jnp.dot(ds, query, preferred_element_type=F32)
                dv = jnp.dot(p.astype(BF16), cot, preferred_element_type=F32)
                if m == 0 and i == min(blocks - 1, j + 2):
                    acc[to, 0:HD] = dk
                    acc[to, HD:PAIR] = dv
                else:
                    acc[to, 0:HD] += dk
                    acc[to, HD:PAIR] += dv
        done = pl.ds(i * BLK, BLK)
        p_ref[done, 0:HD] = (acc[done, 0:HD] * factor).astype(BF16)
        p_ref[done, HD:PAIR] = acc[done, HD:PAIR].astype(BF16)

        @pl.when(x != i)
        def _(i=i):
            block_copy(i).start()

    loads[3].wait()
    starts = [0] + ends[:3]
    for hf in range(2):
        o = 2 * BLK * hf
        turned = jnp.concatenate(
            [
                x_ref[o : o + CUT],
                x_ref[o + BLK : o + BLK + CUT],
                x_ref[o + CUT : o + BLK],
                x_ref[o + BLK + CUT : o + 2 * BLK],
            ],
            axis=0,
        ).T
        pos = lax.broadcasted_iota(jnp.int32, (1, 2 * BLK), 1)
        late = pos - 2 * CUT
        token = o + jnp.where(
            pos < 2 * CUT,
            pos + jnp.where(pos >= CUT, BLK - CUT, 0),
            late + CUT + jnp.where(late >= REST, BLK - REST, 0),
        )
        for n in range(3):
            s = hf + n
            inside = jnp.where((token >= starts[s]) & (token < ends[s]), 1.0, 0.0).astype(BF16)
            masked = turned * inside
            for rb in range(2):
                xm[rb, hf, n * HD : (n + 1) * HD, :] = masked[rb * HD : (rb + 1) * HD]
    loads[4].wait()

    def cut_rows(q):
        return (q // 2, pl.ds(pl.multiple_of(CUT * (q % 2), CUT), CUT))

    def rest_rows(q):
        return (q // 2, pl.ds(pl.multiple_of(2 * CUT + REST * (q % 2), 32), REST))

    summed = p_ref[pl.ds(pl.multiple_of(x * BLK, BLK), BLK), :].astype(F32)
    for by in range(3):
        pltpu.make_async_remote_copy(
            src_ref=p_ref.at[0:BLK],
            dst_ref=rs_in.at[by],
            send_sem=block_send.at[0],
            recv_sem=block_recv.at[by],
            device_id=at.along_x(1),
            device_id_type=MESH,
        ).wait_recv()
        summed = summed + rs_in[by].astype(F32)
    summed = summed.astype(BF16)
    hf, r = cut_rows(x)
    g[z, hf, r, :] = summed[:CUT]
    hf, r = rest_rows(x)
    g[z, hf, r, :] = summed[CUT:]

    def ring_piece(h, place, base, size, part):
        q = (x + place) % 4
        unit = size // 2
        length = size if part is None else unit
        skip = 0 if part is None else part * unit
        start = pl.multiple_of(base + size * (q % 2) + skip, 16)
        return g.at[h, q // 2, pl.ds(start, length)]

    def around_copy(piece, way):
        return send.start(piece, piece, at.along_x(way), spare.pop(0) if spare else None)

    class AroundX:
        def __init__(self, h, base, size):
            self.h, self.base, self.size = h, base, size
            own = ring_piece(h, 0, base, size, None)
            self.up = around_copy(own, 1)
            self.down = around_copy(own, -1)

        def pass_on(self):
            self.up.wait_recv()
            piece = ring_piece(self.h, 3, self.base, self.size, 0)
            self.up2 = around_copy(piece, 1)
            self.down.wait_recv()
            piece = ring_piece(self.h, 1, self.base, self.size, 1)
            self.down2 = around_copy(piece, -1)

        def end(self):
            self.up2.wait_recv()
            self.down2.wait_recv()

    def head(k):
        return (z + k + 8) % 8

    def send_rest(h, way):
        hf, r = rest_rows(x)
        piece = g.at[h, hf, r]
        return send.start(piece, piece, at.along_z(way))

    def send_cut(h, hf, way):
        piece = g.at[h, hf, 0 : 2 * CUT]
        return send.start(piece, piece, at.along_z(way))

    heads = [0, -1, 1, -2, 2, -3, 3, 4]

    def fisher_rows(slot, h, rb):
        a = jnp.dot(xm[rb, 0], g[h, 0], preferred_element_type=F32)
        b = jnp.dot(xm[rb, 1], g[h, 1], preferred_element_type=F32)
        g0, g3 = a[:HD], b[2 * HD :]
        g1, g2 = a[HD : 2 * HD] + b[:HD], a[2 * HD :] + b[HD : 2 * HD]
        f = g0 * g0 + g1 * g1 + g2 * g2 + g3 * g3
        fb[slot, pl.ds(pl.multiple_of(rb * HD, HD), HD), :] = f
        return f

    def weights(h, rb):
        return w_ref[pl.ds(pl.multiple_of(rb * HD, HD), HD), columns(h)].astype(F32)

    pair, over_y, merged_y, merged_core = {}, {}, {}, {}

    def compute_other(slot):
        h = head(heads[slot])
        rb = 1 - core
        f = fisher_rows(slot, h, rb)
        ps[slot, 0] = (f * weights(h, rb)).astype(BF16)
        ps[slot, 1] = f.astype(BF16)
        pair[slot] = send.start(ps.at[slot], pr.at[slot], at.other_core())

    def compute_own(slot):
        h = head(heads[slot])
        fisher_rows(slot, h, core)
        pltpu.make_async_copy(fb.at[slot], fisher_out.at[:, columns(h)], local_sems.at[6]).start()

    def sum_pair(slot):
        h = head(heads[slot])
        pair[slot].wait_recv()
        f = fb[slot, pl.ds(pl.multiple_of(core * HD, HD), HD), :]
        ys[slot, 0] = (f * weights(h, core) + pr[slot, 0].astype(F32)).astype(BF16)
        ys[slot, 1] = (f + pr[slot, 1].astype(F32)).astype(BF16)
        over_y[slot] = send.fresh()
        for k in (2, 1, 3):
            r = pl.ds(pl.multiple_of(((y + k) % 4) * 32, 32), 32)
            send.start(ys.at[slot, :, r], yr.at[slot, k - 1], at.along_y(k), over_y[slot])

    def divide(slot):
        h = head(heads[slot])
        send.arrived(yr.at[slot], over_y[slot])
        r = pl.ds(pl.multiple_of(y * 32, 32), 32)
        sums = ys[slot, :, r, :].astype(F32)
        for k in range(3):
            sums = sums + yr[slot, k].astype(F32)
        to = pl.ds(pl.multiple_of(core * HD + y * 32, 32), 32)
        mb[h, to, :] = (sums[0] / (sums[1] + EPS)).astype(BF16)
        piece = mb.at[h, to]
        merged_y[slot] = send.fresh()
        for k in (2, 1, 3):
            send.start(piece, piece, at.along_y(k), merged_y[slot])
        if slot == 7:
            for k in (2, 1, 3):
                send.start(piece, piece, at.along_y(k, True), merged_y[slot])
            send.start(piece, piece, at.other_core(), merged_y[slot])

    def share(slot):
        h = head(heads[slot])
        send.arrived(mb.at[h, 0 : 224 if slot == 7 else 96], merged_y[slot])
        if slot < 7:
            piece = mb.at[h, pl.ds(pl.multiple_of(core * HD, HD), HD)]
            merged_core[slot] = send.start(piece, piece, at.other_core())

    def close(slot):
        h = head(heads[slot])
        if slot < 7:
            merged_core[slot].wait_recv()
        pltpu.make_async_copy(mb.at[h], merged_out.at[:, columns(h)], local_sems.at[7]).start()

    rings = {}
    rest = {"up": send_rest(z, 1), "down": send_rest(z, -1)}

    def rest_hop(k):
        if k < 4:
            rest["up"].wait_recv()
            if k < 3:
                rest["up"] = send_rest(head(-k), 1)
        rest["down"].wait_recv()
        if k < 4:
            rest["down"] = send_rest(head(k), -1)

    def around(slot):
        rings[slot] = AroundX(head(heads[slot]), 2 * CUT, REST)

    cut = {}

    def cut_hop(k, hf):
        last_up, last_down = (4, 3) if hf == 0 else (3, 4)
        if k <= last_up:
            cut["up", hf].wait_recv()
            if k < last_up:
                cut["up", hf] = send_cut(head(-k), hf, 1)
        if k <= last_down:
            cut["down", hf].wait_recv()
            if k < last_down:
                cut["down", hf] = send_cut(head(k), hf, -1)

    def further(slot):
        rings[slot].pass_on()
        if slot + 2 < 8:
            around(slot + 2)

    cut_ring = AroundX(z, 0, CUT)
    cut_ring.pass_on()
    around(0)
    rest_hop(1)
    around(1)
    cut_ring.end()
    for hf in range(2):
        for name, way in (("up", 1), ("down", -1)):
            cut[name, hf] = send_cut(z, hf, way)
    further(0)
    rest_hop(2)
    further(1)
    rings[0].end()
    compute_other(0)
    compute_own(0)
    sum_pair(0)
    cut_hop(1, 0)
    for k in range(1, 4):
        a, b = 2 * k - 1, 2 * k
        further(b)
        if k < 3:
            rest_hop(k + 2)
        cut_hop(k, 1)
        rings[a].end()
        compute_other(a)
        compute_own(a)
        further(b + 1)
        for slot in (a - 2, b - 2):
            if slot >= 0:
                divide(slot)
        rings[b].end()
        compute_other(b)
        sum_pair(a)
        compute_own(b)
        sum_pair(b)
        for slot in (a - 4, b - 4):
            if slot >= 0:
                share(slot)
        cut_hop(k + 1, 0)
    cut_hop(4, 1)
    rings[7].end()
    compute_other(7)
    compute_own(7)
    sum_pair(7)
    close(0)
    for slot in (5, 6):
        divide(slot)
    for slot in (3, 4):
        share(slot)
    divide(7)
    for slot in (1, 2):
        close(slot)
    for slot in (5, 6):
        share(slot)
    for slot in (3, 4):
        close(slot)
    share(7)
    for slot in (7, 5, 6):
        close(slot)
    send.finish()
    pltpu.make_async_copy(fb, fb, local_sems.at[6]).wait()
    pltpu.make_async_copy(mb, mb, local_sems.at[7]).wait()
    for j in range(blocks):

        @pl.when(x != j)
        def _(j=j):
            block_copy(j).wait_send()


def write_kernel(fisher_ref, merged_ref, fisher_out, merged_out, fisher, merged, in_sems, out_sems):
    copies = []
    for n in range(8):
        src, held, dst = (
            (fisher_ref, fisher, fisher_out) if n < 4 else (merged_ref, merged, merged_out)
        )
        r = pl.ds((n % 4) * (BLK // 4), BLK // 4)
        copies.append(
            (
                pltpu.make_async_copy(src.at[r], held.at[r], in_sems.at[n]),
                pltpu.make_async_copy(held.at[r], dst.at[r], out_sems.at[n]),
            )
        )
    for come, go in copies:
        come.start()
    for come, go in copies:
        come.wait()
        go.start()
    for come, go in copies:
        go.wait()


def body(layer_inputs, queries, key_values, out_grads, lengths, task_weights):
    hbm = pl.BlockSpec(memory_space=pl.ANY)
    wide = KVH * PAIR
    results = (
        jax.ShapeDtypeStruct((BLK, wide), F32),
        jax.ShapeDtypeStruct((BLK, wide), BF16),
    )
    fisher, merged = pl.pallas_call(
        step_kernel,
        out_shape=results,
        in_specs=[hbm] * 5 + [pl.BlockSpec(memory_space=pltpu.SMEM)],
        out_specs=(hbm, hbm),
        scratch_shapes=[
            pltpu.VMEM((TOK // 32, wide), BF16),
            pltpu.VMEM((TOK, PAIR), BF16),
            pltpu.VMEM((TOK, PAIR), BF16),
            pltpu.VMEM((TOK, BLK), BF16),
            pltpu.VMEM((BLK, wide), BF16),
            pltpu.VMEM((TOK, PAIR), BF16),
            pltpu.VMEM((3, BLK, BLK), F32),
            pltpu.VMEM((3, BLK, BLK), F32),
            pltpu.VMEM((TOK, PAIR), F32),
            pltpu.VMEM((TOK, PAIR), BF16),
            pltpu.VMEM((3, BLK, PAIR), BF16),
            pltpu.VMEM((2, 2, 3 * HD, 2 * BLK), BF16),
            pltpu.VMEM((KVH, 2, 2 * BLK, PAIR), BF16),
            pltpu.VMEM((8, BLK, PAIR), F32),
            pltpu.VMEM((8, 2, HD, PAIR), BF16),
            pltpu.VMEM((8, 2, HD, PAIR), BF16),
            pltpu.VMEM((8, 2, HD, PAIR), BF16),
            pltpu.VMEM((8, 3, 2, 32, PAIR), BF16),
            pltpu.VMEM((KVH, BLK, PAIR), BF16),
            pltpu.SemaphoreType.DMA((TURNS,)),
            pltpu.SemaphoreType.DMA((SEMS,)),
            pltpu.SemaphoreType.DMA((4,)),
            pltpu.SemaphoreType.DMA((3,)),
            pltpu.SemaphoreType.DMA((8,)),
        ],
        compiler_params=pltpu.CompilerParams(collective_id=0, has_side_effects=True),
        name="step",
    )(key_values[0], queries[0], out_grads[0], layer_inputs[0], task_weights[0], lengths)
    fisher, merged = pl.pallas_call(
        write_kernel,
        out_shape=results,
        in_specs=[hbm, hbm],
        out_specs=(hbm, hbm),
        scratch_shapes=[
            pltpu.VMEM((BLK, wide), F32),
            pltpu.VMEM((BLK, wide), BF16),
            pltpu.SemaphoreType.DMA((8,)),
            pltpu.SemaphoreType.DMA((8,)),
        ],
        name="write",
    )(fisher, merged)
    return fisher[None], merged


def solution(mesh):
    placed = (
        P("task", None, "col"),
        P("task", None, "col"),
        P("task", "col", None),
        P("task", None, "col"),
        P("task", None),
        P("task", "col", None),
    )
    return jax.shard_map(
        body,
        mesh=mesh,
        in_specs=placed,
        out_specs=(P("task", "col", None), P("col", None)),
        check_vma=False,
    )
```

```python
import functools

import jax
import jax.numpy as jnp
from jax import lax
from jax.experimental import pallas as pl
from jax.experimental.pallas import tpu as pltpu
from jax.sharding import PartitionSpec as P

MESH = pl.DeviceIdType.MESH
F32, BF16 = jnp.float32, jnp.bfloat16
KVH = 8
HD = 128
PAIR = 2 * HD
TOK = 1024
BLK = 256
OWN = BLK // 4
CUT = 48
REST = 2 * OWN - CUT
EPS = 1e-06
NEGATIVE = -1e30
TURNS = 24
SEMS = 96


class Where:
    def __init__(self):
        self.task, self.col = lax.axis_index("task"), lax.axis_index("col")
        self.y, self.core = self.task // 2, self.task % 2
        self.z, self.x = self.col // 4, self.col % 4

    def along_x(self, by):
        return (self.task, self.z * 4 + (self.x + by + 4) % 4)

    def along_z(self, by):
        return (self.task, ((self.z + by + 8) % 8) * 4 + self.x)

    def along_y(self, by, across=False):
        core = 1 - self.core if across else self.core
        return (((self.y + by) % 4) * 2 + core, self.col)

    def other_core(self):
        return (self.y * 2 + 1 - self.core, self.col)


def meet(devices):
    barrier = pltpu.get_barrier_semaphore()
    for device in devices:
        pl.semaphore_signal(barrier, inc=1, device_id=device, device_id_type=MESH)
    pl.semaphore_wait(barrier, len(devices))


class Sender:
    def __init__(self, send_sems, recv_sems):
        self.send_sems, self.recv_sems = send_sems, recv_sems
        self.copies, self.used = [], 0

    def fresh(self):
        self.used += 1
        assert self.used <= SEMS
        return self.recv_sems.at[self.used - 1]

    def start(self, src, dst, device, recv_sem=None):
        at = len(self.copies)
        if at >= TURNS:
            self.copies[at - TURNS].wait_send()
        copy = pltpu.make_async_remote_copy(
            src_ref=src,
            dst_ref=dst,
            send_sem=self.send_sems.at[at % TURNS],
            recv_sem=self.fresh() if recv_sem is None else recv_sem,
            device_id=device,
            device_id_type=MESH,
        )
        copy.start()
        self.copies.append(copy)
        return copy

    def arrived(self, ref, recv_sem):
        pltpu.make_async_remote_copy(
            src_ref=ref,
            dst_ref=ref,
            send_sem=self.send_sems.at[0],
            recv_sem=recv_sem,
            device_id=(0, 0),
            device_id_type=MESH,
        ).wait_recv()

    def finish(self):
        for copy in self.copies[-TURNS:]:
            copy.wait_send()


def bounds(lengths_ref):
    ends, end = [], 0
    for s in range(4):
        end = end + lengths_ref[0, s]
        ends.append(end)
    return ends


def dot_nt(a, b):
    return lax.dot_general(a, b, (((1,), (1,)), ((), ())), preferred_element_type=F32)


def step_kernel(
    kv_hbm,
    q_hbm,
    og_hbm,
    x_hbm,
    w_hbm,
    len_ref,
    fisher_out,
    merged_out,
    kv_ref,
    q_ref,
    og_ref,
    x_ref,
    w_ref,
    kv,
    score,
    slope,
    acc,
    p_ref,
    rs_in,
    xm,
    g,
    fb,
    ps,
    pr,
    ys,
    yr,
    mb,
    send_sems,
    recv_sems,
    local_sems,
):
    at = Where()
    send = Sender(send_sems, recv_sems)
    x, z, y, core = at.x, at.z, at.y, at.core

    loads = []
    for n, (src, dst) in enumerate(
        ((kv_hbm, kv_ref), (q_hbm, q_ref), (og_hbm, og_ref), (x_hbm, x_ref), (w_hbm, w_ref))
    ):
        copy = pltpu.make_async_copy(src, dst, local_sems.at[n])
        copy.start()
        loads.append(copy)
    meet(
        [at.along_z(k) for k in (4, 3, 5, 2, 6, 1, 7)]
        + [at.along_y(k) for k in (2, 1, 3)]
        + [at.along_y(k, True) for k in (2, 1, 3)]
        + [at.along_x(2), at.along_x(1), at.along_x(-1), at.other_core()]
    )

    def rows(z, x):
        return pl.ds(pl.multiple_of(z * 128 + x * 32, 32), 32)

    def columns(h):
        return pl.ds(pl.multiple_of(h * PAIR, PAIR), PAIR)

    loads[0].wait()
    own = pltpu.make_async_copy(kv_ref.at[:, columns(z)], kv.at[rows(z, x)], local_sems.at[5])
    own.start()
    steps = (1, 7, 2, 6, 3, 5, 4)
    spare = {k: send.fresh() for k in steps}
    arrive = {
        k: send.start(kv_ref.at[:, columns((z + k) % 8)], kv.at[rows(z, x)], at.along_z(k), spare[k])
        for k in steps
    }
    spare = list(spare.values())
    spread = []

    def spread_block(z):
        block = kv.at[rows(z, x)]
        for by in (2, 1, -1):
            spare.append(send.fresh())
            spread.append(send.start(block, block, at.along_x(by), spare[-1]))

    own.wait()
    spread_block(z)
    for k in steps:
        arrive[k].wait_recv()
        spread_block((z + 8 - k) % 8)
    for copy in loads[1:3]:
        copy.wait()
    for copy in spread:
        copy.wait_recv()

    factor = HD**-0.5
    ends = bounds(len_ref)
    blocks = TOK // BLK

    def piece_of(j, by):
        return pl.ds(pl.multiple_of(j * BLK + ((x + by + 4) % 4) * OWN, OWN), OWN)

    block_sems = [send.fresh() for j in range(blocks)]

    def send_block(j):
        for by in (2, 1, 3):
            send.start(p_ref.at[piece_of(j, by)], rs_in.at[j, by - 1], at.along_x(by), block_sems[j])

    for i in reversed(range(blocks)):
        queries = pl.ds(i * BLK, BLK)
        low = max(0, i - 2)
        token = i * BLK + lax.broadcasted_iota(jnp.int32, (1, BLK), 1)
        opening = jnp.zeros_like(token)
        for s in range(3):
            opening = jnp.where(token >= ends[s], ends[s], opening)
        for m in range(2):
            lanes = pl.ds(m * HD, HD)
            query = q_ref[queries, lanes]
            cot = og_ref[queries, lanes]
            highest = jnp.full((1, BLK), NEGATIVE, F32)
            for j in range(low, i + 1):
                key = kv[pl.ds(j * BLK, BLK), 0:HD]
                place = j * BLK + lax.broadcasted_iota(jnp.int32, (BLK, BLK), 0)
                allowed = place >= opening
                if j == i:
                    allowed = allowed & (place <= token)
                s = jnp.where(allowed, dot_nt(key, query) * factor, NEGATIVE)
                score[j - low] = s
                highest = jnp.maximum(highest, jnp.max(s, axis=0, keepdims=True))
            total = jnp.zeros((1, BLK), F32)
            weighed = jnp.zeros((1, BLK), F32)
            for j in range(low, i + 1):
                e = jnp.exp(score[j - low] - highest)
                score[j - low] = e
                d = dot_nt(kv[pl.ds(j * BLK, BLK), HD:PAIR], cot)
                slope[j - low] = d
                total = total + jnp.sum(e, axis=0, keepdims=True)
                weighed = weighed + jnp.sum(e * d, axis=0, keepdims=True)
            inverse = 1.0 / total
            offset = weighed * inverse
            for j in range(low, i + 1):
                p = score[j - low] * inverse
                ds = (p * (slope[j - low] - offset)).astype(BF16)
                to = pl.ds(j * BLK, BLK)
                dk = jnp.dot(ds, query, preferred_element_type=F32)
                dv = jnp.dot(p.astype(BF16), cot, preferred_element_type=F32)
                if m == 0 and i == min(blocks - 1, j + 2):
                    acc[to, 0:HD] = dk
                    acc[to, HD:PAIR] = dv
                else:
                    acc[to, 0:HD] += dk
                    acc[to, HD:PAIR] += dv
        done = pl.ds(i * BLK, BLK)
        p_ref[done, 0:HD] = (acc[done, 0:HD] * factor).astype(BF16)
        p_ref[done, HD:PAIR] = acc[done, HD:PAIR].astype(BF16)
        send_block(i)

    loads[3].wait()
    starts = [0] + ends[:3]
    for hf in range(2):
        o = 2 * BLK * hf
        early = [x_ref[o + OWN * q : o + OWN * q + CUT] for q in range(4)]
        late = []
        for q in range(4):
            late.append(x_ref[o + OWN * q + CUT : o + OWN * q + OWN])
            late.append(x_ref[o + BLK + OWN * q : o + BLK + OWN * q + OWN])
        turned = jnp.concatenate(early + late, axis=0).T
        pos = lax.broadcasted_iota(jnp.int32, (1, 2 * BLK), 1)
        token = jnp.zeros_like(pos)
        for q in range(4):
            token = jnp.where(pos >= CUT * q, pos - CUT * q + OWN * q, token)
        for q in range(4):
            base = 4 * CUT + REST * q
            token = jnp.where(pos >= base, pos - base + CUT + OWN * q, token)
            base += OWN - CUT
            token = jnp.where(pos >= base, pos - base + BLK + OWN * q, token)
        token = token + o
        for n in range(3):
            s = hf + n
            inside = jnp.where((token >= starts[s]) & (token < ends[s]), 1.0, 0.0).astype(BF16)
            masked = turned * inside
            for rb in range(2):
                xm[rb, hf, n * HD : (n + 1) * HD, :] = masked[rb * HD : (rb + 1) * HD]
    loads[4].wait()

    def cut_rows(q):
        return pl.ds(pl.multiple_of(CUT * (q % 4), CUT), CUT)

    def rest_rows(q, skip=0, length=REST):
        return pl.ds(pl.multiple_of(4 * CUT + REST * (q % 4) + skip, 16), length)

    def settle(j):
        send.arrived(rs_in.at[j], block_sems[j])
        summed = p_ref[piece_of(j, 0), :].astype(F32)
        for by in range(3):
            summed = summed + rs_in[j, by].astype(F32)
        summed = summed.astype(BF16)
        if j % 2 == 0:
            g[z, j // 2, cut_rows(x), :] = summed[:CUT]
            g[z, j // 2, rest_rows(x, 0, OWN - CUT), :] = summed[CUT:]
        else:
            g[z, j // 2, rest_rows(x, OWN - CUT, OWN), :] = summed

    def around_copy(piece, way):
        return send.start(piece, piece, at.along_x(way), spare.pop(0) if spare else None)

    class Ring:
        def __init__(self, h):
            self.h = h
            own = g.at[h, :, rest_rows(x)]
            self.up = around_copy(own, 1)
            self.down = around_copy(own, -1)

        def pass_on(self):
            self.up.wait_recv()
            self.up2 = around_copy(g.at[self.h, 0, rest_rows(x + 3)], 1)
            self.down.wait_recv()
            self.down2 = around_copy(g.at[self.h, 1, rest_rows(x + 1)], -1)

        def end(self):
            self.up2.wait_recv()
            self.down2.wait_recv()

    def head(k):
        return (z + k + 8) % 8

    def send_rest(h, way):
        piece = g.at[h, :, rest_rows(x)]
        return send.start(piece, piece, at.along_z(way))

    def send_cut(h, hf, way):
        piece = g.at[h, hf, 0 : 4 * CUT]
        return send.start(piece, piece, at.along_z(way))

    heads = [0, -1, 1, -2, 2, -3, 3, 4]

    def fisher_rows(slot, h, rb):
        a = jnp.dot(xm[rb, 0], g[h, 0], preferred_element_type=F32)
        b = jnp.dot(xm[rb, 1], g[h, 1], preferred_element_type=F32)
        g0, g3 = a[:HD], b[2 * HD :]
        g1, g2 = a[HD : 2 * HD] + b[:HD], a[2 * HD :] + b[HD : 2 * HD]
        f = g0 * g0 + g1 * g1 + g2 * g2 + g3 * g3
        fb[slot, pl.ds(pl.multiple_of(rb * HD, HD), HD), :] = f
        return f

    def weights(h, rb):
        return w_ref[pl.ds(pl.multiple_of(rb * HD, HD), HD), columns(h)].astype(F32)

    pair, over_y, merged_y, merged_core = {}, {}, {}, {}

    def compute_other(slot):
        h = head(heads[slot])
        rb = 1 - core
        f = fisher_rows(slot, h, rb)
        ps[slot, 0] = (f * weights(h, rb)).astype(BF16)
        ps[slot, 1] = f.astype(BF16)
        pair[slot] = send.start(ps.at[slot], pr.at[slot], at.other_core())

    def compute_own(slot):
        h = head(heads[slot])
        fisher_rows(slot, h, core)
        pltpu.make_async_copy(fb.at[slot], fisher_out.at[:, columns(h)], local_sems.at[6]).start()

    def sum_pair(slot):
        h = head(heads[slot])
        pair[slot].wait_recv()
        f = fb[slot, pl.ds(pl.multiple_of(core * HD, HD), HD), :]
        ys[slot, 0] = (f * weights(h, core) + pr[slot, 0].astype(F32)).astype(BF16)
        ys[slot, 1] = (f + pr[slot, 1].astype(F32)).astype(BF16)
        over_y[slot] = send.fresh()
        for k in (2, 1, 3):
            r = pl.ds(pl.multiple_of(((y + k) % 4) * 32, 32), 32)
            send.start(ys.at[slot, :, r], yr.at[slot, k - 1], at.along_y(k), over_y[slot])

    def divide(slot):
        h = head(heads[slot])
        send.arrived(yr.at[slot], over_y[slot])
        r = pl.ds(pl.multiple_of(y * 32, 32), 32)
        sums = ys[slot, :, r, :].astype(F32)
        for k in range(3):
            sums = sums + yr[slot, k].astype(F32)
        to = pl.ds(pl.multiple_of(core * HD + y * 32, 32), 32)
        mb[h, to, :] = (sums[0] / (sums[1] + EPS)).astype(BF16)
        piece = mb.at[h, to]
        merged_y[slot] = send.fresh()
        for k in (2, 1, 3):
            send.start(piece, piece, at.along_y(k), merged_y[slot])
        if slot == 7:
            for k in (2, 1, 3):
                send.start(piece, piece, at.along_y(k, True), merged_y[slot])
            send.start(piece, piece, at.other_core(), merged_y[slot])

    def share(slot):
        h = head(heads[slot])
        send.arrived(mb.at[h, 0 : 224 if slot == 7 else 96], merged_y[slot])
        if slot < 7:
            piece = mb.at[h, pl.ds(pl.multiple_of(core * HD, HD), HD)]
            merged_core[slot] = send.start(piece, piece, at.other_core())

    def close(slot):
        h = head(heads[slot])
        if slot < 7:
            merged_core[slot].wait_recv()
        pltpu.make_async_copy(mb.at[h], merged_out.at[:, columns(h)], local_sems.at[7]).start()

    rings = {}
    rest = {}
    rest_first = {"up": send.fresh(), "down": send.fresh()}
    ways = (("up", 1), ("down", -1))

    def rest_arrives(name, k):
        if k == 1:
            send.arrived(g.at[z, :, rest_rows(x)], rest_first[name])
        else:
            rest[name].wait_recv()

    def rest_hop(k):
        if k < 4:
            rest_arrives("up", k)
            if k < 3:
                rest["up"] = send_rest(head(-k), 1)
        rest_arrives("down", k)
        if k < 4:
            rest["down"] = send_rest(head(k), -1)

    def around(slot):
        rings[slot] = Ring(head(heads[slot]))

    cut = {}

    def cut_hop(k, hf):
        last_up, last_down = (4, 3) if hf == 0 else (3, 4)
        if k <= last_up:
            cut["up", hf].wait_recv()
            if k < last_up:
                cut["up", hf] = send_cut(head(-k), hf, 1)
        if k <= last_down:
            cut["down", hf].wait_recv()
            if k < last_down:
                cut["down", hf] = send_cut(head(k), hf, -1)

    def further(slot):
        rings[slot].pass_on()
        if slot + 2 < 8:
            around(slot + 2)

    cut_ring = {}
    for hf in (1, 0):
        settle(2 * hf + 1)
        settle(2 * hf)
        for name, way in ways:
            piece = g.at[z, hf, cut_rows(x)]
            cut_ring[name, hf] = around_copy(piece, way)
        for name, way in ways:
            piece = g.at[z, hf, rest_rows(x)]
            send.start(piece, piece, at.along_z(way), rest_first[name])
    cut_ring["up", 1].wait_recv()
    far_up = around_copy(g.at[z, 1, cut_rows(x + 3)], 1)
    cut_ring["down", 0].wait_recv()
    far_down = around_copy(g.at[z, 0, cut_rows(x + 1)], -1)
    around(0)
    rest_hop(1)
    around(1)
    cut_ring["down", 1].wait_recv()
    far_up.wait_recv()
    for name, way in ways:
        cut[name, 1] = send_cut(z, 1, way)
    cut_ring["up", 0].wait_recv()
    far_down.wait_recv()
    for name, way in ways:
        cut[name, 0] = send_cut(z, 0, way)
    further(0)
    rest_hop(2)
    further(1)
    for slot in range(8):
        rings[slot].end()
        compute_other(slot)
        compute_own(slot)
        if slot + 2 < 8:
            further(slot + 2)
        if slot in (0, 2):
            rest_hop(slot // 2 + 3)
        if slot % 2 == 0 and slot < 7:
            cut_hop(slot // 2 + 1, 1)
            cut_hop(slot // 2 + 1, 0)
        sum_pair(slot)
        if slot >= 2:
            divide(slot - 2)
        if slot >= 4:
            share(slot - 4)
    divide(6)
    share(4)
    close(0)
    close(1)
    divide(7)
    close(2)
    share(5)
    close(3)
    close(4)
    share(6)
    share(7)
    for slot in (7, 5, 6):
        close(slot)
    send.finish()
    pltpu.make_async_copy(fb, fb, local_sems.at[6]).wait()
    pltpu.make_async_copy(mb, mb, local_sems.at[7]).wait()


def write_kernel(fisher_ref, merged_ref, fisher_out, merged_out, fisher, merged, in_sems, out_sems):
    copies = []
    for n in range(8):
        src, held, dst = (
            (fisher_ref, fisher, fisher_out) if n < 4 else (merged_ref, merged, merged_out)
        )
        r = pl.ds((n % 4) * (BLK // 4), BLK // 4)
        copies.append(
            (
                pltpu.make_async_copy(src.at[r], held.at[r], in_sems.at[n]),
                pltpu.make_async_copy(held.at[r], dst.at[r], out_sems.at[n]),
            )
        )
    for come, go in copies:
        come.start()
    for come, go in copies:
        come.wait()
        go.start()
    for come, go in copies:
        go.wait()


def body(layer_inputs, queries, key_values, out_grads, lengths, task_weights):
    hbm = pl.BlockSpec(memory_space=pl.ANY)
    wide = KVH * PAIR
    results = (
        jax.ShapeDtypeStruct((BLK, wide), F32),
        jax.ShapeDtypeStruct((BLK, wide), BF16),
    )
    fisher, merged = pl.pallas_call(
        step_kernel,
        out_shape=results,
        in_specs=[hbm] * 5 + [pl.BlockSpec(memory_space=pltpu.SMEM)],
        out_specs=(hbm, hbm),
        scratch_shapes=[
            pltpu.VMEM((TOK // 32, wide), BF16),
            pltpu.VMEM((TOK, PAIR), BF16),
            pltpu.VMEM((TOK, PAIR), BF16),
            pltpu.VMEM((TOK, BLK), BF16),
            pltpu.VMEM((BLK, wide), BF16),
            pltpu.VMEM((TOK, PAIR), BF16),
            pltpu.VMEM((3, BLK, BLK), F32),
            pltpu.VMEM((3, BLK, BLK), F32),
            pltpu.VMEM((TOK, PAIR), F32),
            pltpu.VMEM((TOK, PAIR), BF16),
            pltpu.VMEM((4, 3, OWN, PAIR), BF16),
            pltpu.VMEM((2, 2, 3 * HD, 2 * BLK), BF16),
            pltpu.VMEM((KVH, 2, 2 * BLK, PAIR), BF16),
            pltpu.VMEM((8, BLK, PAIR), F32),
            pltpu.VMEM((8, 2, HD, PAIR), BF16),
            pltpu.VMEM((8, 2, HD, PAIR), BF16),
            pltpu.VMEM((8, 2, HD, PAIR), BF16),
            pltpu.VMEM((8, 3, 2, 32, PAIR), BF16),
            pltpu.VMEM((KVH, BLK, PAIR), BF16),
            pltpu.SemaphoreType.DMA((TURNS,)),
            pltpu.SemaphoreType.DMA((SEMS,)),
            pltpu.SemaphoreType.DMA((8,)),
        ],
        compiler_params=pltpu.CompilerParams(collective_id=0, has_side_effects=True),
        name="step",
    )(key_values[0], queries[0], out_grads[0], layer_inputs[0], task_weights[0], lengths)
    fisher, merged = pl.pallas_call(
        write_kernel,
        out_shape=results,
        in_specs=[hbm, hbm],
        out_specs=(hbm, hbm),
        scratch_shapes=[
            pltpu.VMEM((BLK, wide), F32),
            pltpu.VMEM((BLK, wide), BF16),
            pltpu.SemaphoreType.DMA((8,)),
            pltpu.SemaphoreType.DMA((8,)),
        ],
        name="write",
    )(fisher, merged)
    return fisher[None], merged


def solution(mesh):
    placed = (
        P("task", None, "col"),
        P("task", None, "col"),
        P("task", "col", None),
        P("task", None, "col"),
        P("task", None),
        P("task", "col", None),
    )
    return jax.shard_map(
        body,
        mesh=mesh,
        in_specs=placed,
        out_specs=(P("task", "col", None), P("col", None)),
        check_vma=False,
    )
```

```python
import functools

import jax
import jax.numpy as jnp
from jax import lax
from jax.experimental import pallas as pl
from jax.experimental.pallas import tpu as pltpu
from jax.sharding import PartitionSpec as P

MESH = pl.DeviceIdType.MESH
F32, BF16 = jnp.float32, jnp.bfloat16
KVH = 8
HD = 128
PAIR = 2 * HD
TOK = 1024
BLK = 256
OWN = BLK // 4
CUT = 48
REST = 2 * OWN - CUT
EPS = 1e-06
NEGATIVE = -1e30
TURNS = 24
SEMS = 96


class Where:
    def __init__(self):
        self.task, self.col = lax.axis_index("task"), lax.axis_index("col")
        self.y, self.core = self.task // 2, self.task % 2
        self.z, self.x = self.col // 4, self.col % 4

    def along_x(self, by):
        return (self.task, self.z * 4 + (self.x + by + 4) % 4)

    def along_z(self, by):
        return (self.task, ((self.z + by + 8) % 8) * 4 + self.x)

    def along_y(self, by, across=False):
        core = 1 - self.core if across else self.core
        return (((self.y + by) % 4) * 2 + core, self.col)

    def other_core(self):
        return (self.y * 2 + 1 - self.core, self.col)


def meet(devices):
    barrier = pltpu.get_barrier_semaphore()
    for device in devices:
        pl.semaphore_signal(barrier, inc=1, device_id=device, device_id_type=MESH)
    pl.semaphore_wait(barrier, len(devices))


class Sender:
    def __init__(self, send_sems, recv_sems):
        self.send_sems, self.recv_sems = send_sems, recv_sems
        self.copies, self.used = [], 0

    def fresh(self):
        self.used += 1
        assert self.used <= SEMS
        return self.recv_sems.at[self.used - 1]

    def start(self, src, dst, device, recv_sem=None):
        at = len(self.copies)
        if at >= TURNS:
            self.copies[at - TURNS].wait_send()
        copy = pltpu.make_async_remote_copy(
            src_ref=src,
            dst_ref=dst,
            send_sem=self.send_sems.at[at % TURNS],
            recv_sem=self.fresh() if recv_sem is None else recv_sem,
            device_id=device,
            device_id_type=MESH,
        )
        copy.start()
        self.copies.append(copy)
        return copy

    def arrived(self, ref, recv_sem):
        pltpu.make_async_remote_copy(
            src_ref=ref,
            dst_ref=ref,
            send_sem=self.send_sems.at[0],
            recv_sem=recv_sem,
            device_id=(0, 0),
            device_id_type=MESH,
        ).wait_recv()

    def finish(self):
        for copy in self.copies[-TURNS:]:
            copy.wait_send()


def bounds(lengths_ref):
    ends, end = [], 0
    for s in range(4):
        end = end + lengths_ref[0, s]
        ends.append(end)
    return ends


def dot_nt(a, b):
    return lax.dot_general(a, b, (((1,), (1,)), ((), ())), preferred_element_type=F32)


def step_kernel(
    kv_hbm,
    q_hbm,
    og_hbm,
    x_hbm,
    w_hbm,
    len_ref,
    fisher_out,
    merged_out,
    kv_ref,
    q_ref,
    og_ref,
    x_ref,
    w_ref,
    kv,
    score,
    slope,
    acc,
    p_ref,
    rs_in,
    xm,
    g,
    fb,
    ps,
    pr,
    ys,
    yr,
    mb,
    send_sems,
    recv_sems,
    local_sems,
):
    at = Where()
    send = Sender(send_sems, recv_sems)
    x, z, y, core = at.x, at.z, at.y, at.core

    loads = []
    for n, (src, dst) in enumerate(
        ((kv_hbm, kv_ref), (q_hbm, q_ref), (og_hbm, og_ref), (x_hbm, x_ref), (w_hbm, w_ref))
    ):
        copy = pltpu.make_async_copy(src, dst, local_sems.at[n])
        copy.start()
        loads.append(copy)
    meet(
        [at.along_z(k) for k in (4, 3, 5, 2, 6, 1, 7)]
        + [at.along_y(k) for k in (2, 1, 3)]
        + [at.along_y(k, True) for k in (2, 1, 3)]
        + [at.along_x(2), at.along_x(1), at.along_x(-1), at.other_core()]
    )

    def rows(z, x):
        return pl.ds(pl.multiple_of(z * 128 + x * 32, 32), 32)

    def columns(h):
        return pl.ds(pl.multiple_of(h * PAIR, PAIR), PAIR)

    loads[0].wait()
    own = pltpu.make_async_copy(kv_ref.at[:, columns(z)], kv.at[rows(z, x)], local_sems.at[5])
    own.start()
    steps = (1, 7, 2, 6, 3, 5, 4)
    spare = {k: send.fresh() for k in steps}
    arrive = {
        k: send.start(kv_ref.at[:, columns((z + k) % 8)], kv.at[rows(z, x)], at.along_z(k), spare[k])
        for k in steps
    }
    spare = list(spare.values())
    spread = []

    def spread_block(z):
        block = kv.at[rows(z, x)]
        for by in (2, 1, -1):
            spare.append(send.fresh())
            spread.append(send.start(block, block, at.along_x(by), spare[-1]))

    own.wait()
    spread_block(z)
    for k in steps:
        arrive[k].wait_recv()
        spread_block((z + 8 - k) % 8)
    for copy in loads[1:3]:
        copy.wait()
    for copy in spread:
        copy.wait_recv()

    factor = HD**-0.5
    ends = bounds(len_ref)
    blocks = TOK // BLK

    def piece_of(j, by):
        return pl.ds(pl.multiple_of(j * BLK + ((x + by + 4) % 4) * OWN, OWN), OWN)

    block_sems = [send.fresh() for j in range(blocks)]

    def send_block(j):
        for by in (2, 1, 3):
            send.start(p_ref.at[piece_of(j, by)], rs_in.at[j, by - 1], at.along_x(by), block_sems[j])

    for i in reversed(range(blocks)):
        queries = pl.ds(i * BLK, BLK)
        low = max(0, i - 2)
        token = i * BLK + lax.broadcasted_iota(jnp.int32, (1, BLK), 1)
        opening = jnp.zeros_like(token)
        for s in range(3):
            opening = jnp.where(token >= ends[s], ends[s], opening)
        heads_in = [
            (q_ref[queries, m * HD : m * HD + HD], og_ref[queries, m * HD : m * HD + HD])
            for m in range(2)
        ]
        highest = [jnp.full((1, BLK), NEGATIVE, F32)] * 2
        for j in range(low, i + 1):
            key = kv[pl.ds(j * BLK, BLK), 0:HD]
            place = j * BLK + lax.broadcasted_iota(jnp.int32, (BLK, BLK), 0)
            allowed = place >= opening
            if j == i:
                allowed = allowed & (place <= token)
            for m in range(2):
                s = jnp.where(allowed, dot_nt(key, heads_in[m][0]) * factor, NEGATIVE)
                score[m, j - low] = s
                highest[m] = jnp.maximum(highest[m], jnp.max(s, axis=0, keepdims=True))
        total = [jnp.zeros((1, BLK), F32)] * 2
        weighed = [jnp.zeros((1, BLK), F32)] * 2
        for j in range(low, i + 1):
            value = kv[pl.ds(j * BLK, BLK), HD:PAIR]
            for m in range(2):
                e = jnp.exp(score[m, j - low] - highest[m])
                score[m, j - low] = e
                d = dot_nt(value, heads_in[m][1])
                slope[m, j - low] = d
                total[m] = total[m] + jnp.sum(e, axis=0, keepdims=True)
                weighed[m] = weighed[m] + jnp.sum(e * d, axis=0, keepdims=True)
        inverse = [1.0 / total[m] for m in range(2)]
        offset = [weighed[m] * inverse[m] for m in range(2)]
        for j in range(low, i + 1):
            dk, dv = 0.0, 0.0
            to = pl.ds(j * BLK, BLK)
            for m in range(2):
                query, cot = heads_in[m]
                p = score[m, j - low] * inverse[m]
                ds = (p * (slope[m, j - low] - offset[m])).astype(BF16)
                dk = dk + jnp.dot(ds, query, preferred_element_type=F32)
                dv = dv + jnp.dot(p.astype(BF16), cot, preferred_element_type=F32)
            if i == min(blocks - 1, j + 2):
                acc[to, 0:HD] = dk
                acc[to, HD:PAIR] = dv
            else:
                acc[to, 0:HD] += dk
                acc[to, HD:PAIR] += dv
        done = pl.ds(i * BLK, BLK)
        p_ref[done, 0:HD] = (acc[done, 0:HD] * factor).astype(BF16)
        p_ref[done, HD:PAIR] = acc[done, HD:PAIR].astype(BF16)
        send_block(i)

    loads[3].wait()
    starts = [0] + ends[:3]
    for hf in range(2):
        o = 2 * BLK * hf
        early = [x_ref[o + OWN * q : o + OWN * q + CUT] for q in range(4)]
        late = []
        for q in range(4):
            late.append(x_ref[o + OWN * q + CUT : o + OWN * q + OWN])
            late.append(x_ref[o + BLK + OWN * q : o + BLK + OWN * q + OWN])
        turned = jnp.concatenate(early + late, axis=0).T
        pos = lax.broadcasted_iota(jnp.int32, (1, 2 * BLK), 1)
        token = jnp.zeros_like(pos)
        for q in range(4):
            token = jnp.where(pos >= CUT * q, pos - CUT * q + OWN * q, token)
        for q in range(4):
            base = 4 * CUT + REST * q
            token = jnp.where(pos >= base, pos - base + CUT + OWN * q, token)
            base += OWN - CUT
            token = jnp.where(pos >= base, pos - base + BLK + OWN * q, token)
        token = token + o
        for n in range(3):
            s = hf + n
            inside = jnp.where((token >= starts[s]) & (token < ends[s]), 1.0, 0.0).astype(BF16)
            masked = turned * inside
            for rb in range(2):
                xm[rb, hf, n * HD : (n + 1) * HD, :] = masked[rb * HD : (rb + 1) * HD]
    loads[4].wait()

    def cut_rows(q):
        return pl.ds(pl.multiple_of(CUT * (q % 4), CUT), CUT)

    def rest_rows(q, skip=0, length=REST):
        return pl.ds(pl.multiple_of(4 * CUT + REST * (q % 4) + skip, 16), length)

    def settle(j):
        send.arrived(rs_in.at[j], block_sems[j])
        summed = p_ref[piece_of(j, 0), :].astype(F32)
        for by in range(3):
            summed = summed + rs_in[j, by].astype(F32)
        summed = summed.astype(BF16)
        if j % 2 == 0:
            g[z, j // 2, cut_rows(x), :] = summed[:CUT]
            g[z, j // 2, rest_rows(x, 0, OWN - CUT), :] = summed[CUT:]
        else:
            g[z, j // 2, rest_rows(x, OWN - CUT, OWN), :] = summed

    def around_copy(piece, way):
        return send.start(piece, piece, at.along_x(way), spare.pop(0) if spare else None)

    class Ring:
        def __init__(self, h, sems=None):
            self.h, self.sems = h, sems
            own = g.at[h, :, rest_rows(x)]
            if sems is None:
                self.up = around_copy(own, 1)
                self.down = around_copy(own, -1)

        def come(self, name):
            if self.sems is None:
                getattr(self, name).wait_recv()
            else:
                send.arrived(g.at[self.h, :, rest_rows(x)], self.sems[name])

        def pass_on(self):
            self.come("up")
            self.up2 = around_copy(g.at[self.h, 0, rest_rows(x + 3)], 1)
            self.come("down")
            self.down2 = around_copy(g.at[self.h, 1, rest_rows(x + 1)], -1)

        def end(self):
            self.up2.wait_recv()
            self.down2.wait_recv()

    def head(k):
        return (z + k + 8) % 8

    def send_rest(h, way):
        piece = g.at[h, :, rest_rows(x)]
        return send.start(piece, piece, at.along_z(way))

    def send_cut(h, hf, way):
        piece = g.at[h, hf, 0 : 4 * CUT]
        return send.start(piece, piece, at.along_z(way))

    heads = [0, -1, 1, -2, 2, -3, 3, 4]

    def fisher_rows(slot, h, rb):
        a = jnp.dot(xm[rb, 0], g[h, 0], preferred_element_type=F32)
        b = jnp.dot(xm[rb, 1], g[h, 1], preferred_element_type=F32)
        g0, g3 = a[:HD], b[2 * HD :]
        g1, g2 = a[HD : 2 * HD] + b[:HD], a[2 * HD :] + b[HD : 2 * HD]
        f = g0 * g0 + g1 * g1 + g2 * g2 + g3 * g3
        fb[slot, pl.ds(pl.multiple_of(rb * HD, HD), HD), :] = f
        return f

    def weights(h, rb):
        return w_ref[pl.ds(pl.multiple_of(rb * HD, HD), HD), columns(h)].astype(F32)

    pair, over_y, merged_y, merged_core = {}, {}, {}, {}

    def compute_other(slot):
        h = head(heads[slot])
        rb = 1 - core
        f = fisher_rows(slot, h, rb)
        ps[slot, 0] = (f * weights(h, rb)).astype(BF16)
        ps[slot, 1] = f.astype(BF16)
        pair[slot] = send.start(ps.at[slot], pr.at[slot], at.other_core())

    def compute_own(slot):
        h = head(heads[slot])
        fisher_rows(slot, h, core)
        pltpu.make_async_copy(fb.at[slot], fisher_out.at[:, columns(h)], local_sems.at[6]).start()

    def sum_pair(slot):
        h = head(heads[slot])
        pair[slot].wait_recv()
        f = fb[slot, pl.ds(pl.multiple_of(core * HD, HD), HD), :]
        ys[slot, 0] = (f * weights(h, core) + pr[slot, 0].astype(F32)).astype(BF16)
        ys[slot, 1] = (f + pr[slot, 1].astype(F32)).astype(BF16)
        over_y[slot] = send.fresh()
        for k in (2, 1, 3):
            r = pl.ds(pl.multiple_of(((y + k) % 4) * 32, 32), 32)
            send.start(ys.at[slot, :, r], yr.at[slot, k - 1], at.along_y(k), over_y[slot])

    def divide(slot):
        h = head(heads[slot])
        send.arrived(yr.at[slot], over_y[slot])
        r = pl.ds(pl.multiple_of(y * 32, 32), 32)
        sums = ys[slot, :, r, :].astype(F32)
        for k in range(3):
            sums = sums + yr[slot, k].astype(F32)
        to = pl.ds(pl.multiple_of(core * HD + y * 32, 32), 32)
        mb[h, to, :] = (sums[0] / (sums[1] + EPS)).astype(BF16)
        piece = mb.at[h, to]
        merged_y[slot] = send.fresh()
        for k in (2, 1, 3):
            send.start(piece, piece, at.along_y(k), merged_y[slot])
        if slot == 7:
            for k in (2, 1, 3):
                send.start(piece, piece, at.along_y(k, True), merged_y[slot])
            send.start(piece, piece, at.other_core(), merged_y[slot])

    def share(slot):
        h = head(heads[slot])
        send.arrived(mb.at[h, 0 : 224 if slot == 7 else 96], merged_y[slot])
        if slot < 7:
            piece = mb.at[h, pl.ds(pl.multiple_of(core * HD, HD), HD)]
            merged_core[slot] = send.start(piece, piece, at.other_core())

    def close(slot):
        h = head(heads[slot])
        if slot < 7:
            merged_core[slot].wait_recv()
        pltpu.make_async_copy(mb.at[h], merged_out.at[:, columns(h)], local_sems.at[7]).start()

    rings = {}
    rest = {}
    rest_first = {"up": send.fresh(), "down": send.fresh()}
    ways = (("up", 1), ("down", -1))

    def rest_arrives(name, k):
        if k == 1:
            send.arrived(g.at[z, :, rest_rows(x)], rest_first[name])
        else:
            rest[name].wait_recv()

    def rest_hop(k):
        if k < 4:
            rest_arrives("up", k)
            if k < 3:
                rest["up"] = send_rest(head(-k), 1)
        rest_arrives("down", k)
        if k < 4:
            rest["down"] = send_rest(head(k), -1)

    def around(slot):
        rings[slot] = Ring(head(heads[slot]))

    cut = {}

    def cut_hop(k, hf):
        last_up, last_down = (4, 3) if hf == 0 else (3, 4)
        if k <= last_up:
            cut["up", hf].wait_recv()
            if k < last_up:
                cut["up", hf] = send_cut(head(-k), hf, 1)
        if k <= last_down:
            cut["down", hf].wait_recv()
            if k < last_down:
                cut["down", hf] = send_cut(head(k), hf, -1)

    def further(slot):
        rings[slot].pass_on()
        if slot + 2 < 8:
            around(slot + 2)

    cut_ring = {}
    ring_first = {"up": spare.pop(0), "down": spare.pop(0)}
    rings[0] = Ring(z, ring_first)
    for hf in (1, 0):
        settle(2 * hf + 1)
        settle(2 * hf)
        for name, way in ways:
            piece = g.at[z, hf, cut_rows(x)]
            cut_ring[name, hf] = around_copy(piece, way)
        for name, way in ways:
            piece = g.at[z, hf, rest_rows(x)]
            send.start(piece, piece, at.along_z(way), rest_first[name])
        for name, way in ways:
            piece = g.at[z, hf, rest_rows(x)]
            send.start(piece, piece, at.along_x(way), ring_first[name])
    cut_ring["up", 1].wait_recv()
    far_up = around_copy(g.at[z, 1, cut_rows(x + 3)], 1)
    cut_ring["down", 0].wait_recv()
    far_down = around_copy(g.at[z, 0, cut_rows(x + 1)], -1)
    rest_hop(1)
    around(1)
    further(0)
    cut_ring["down", 1].wait_recv()
    far_up.wait_recv()
    for name, way in ways:
        cut[name, 1] = send_cut(z, 1, way)
    cut_ring["up", 0].wait_recv()
    far_down.wait_recv()
    for name, way in ways:
        cut[name, 0] = send_cut(z, 0, way)
    rest_hop(2)
    further(1)
    for slot in range(8):
        rings[slot].end()
        compute_other(slot)
        compute_own(slot)
        if slot + 2 < 8:
            further(slot + 2)
        if slot in (0, 2):
            rest_hop(slot // 2 + 3)
        if slot % 2 == 0 and slot < 7:
            cut_hop(slot // 2 + 1, 1)
            cut_hop(slot // 2 + 1, 0)
        sum_pair(slot)
        if slot >= 2:
            divide(slot - 2)
        if slot >= 4:
            share(slot - 4)
    divide(6)
    share(4)
    close(0)
    close(1)
    divide(7)
    close(2)
    share(5)
    close(3)
    close(4)
    share(6)
    share(7)
    for slot in (7, 5, 6):
        close(slot)
    send.finish()
    pltpu.make_async_copy(fb, fb, local_sems.at[6]).wait()
    pltpu.make_async_copy(mb, mb, local_sems.at[7]).wait()


def write_kernel(fisher_ref, merged_ref, fisher_out, merged_out, fisher, merged, in_sems, out_sems):
    copies = []
    for n in range(8):
        src, held, dst = (
            (fisher_ref, fisher, fisher_out) if n < 4 else (merged_ref, merged, merged_out)
        )
        r = pl.ds((n % 4) * (BLK // 4), BLK // 4)
        copies.append(
            (
                pltpu.make_async_copy(src.at[r], held.at[r], in_sems.at[n]),
                pltpu.make_async_copy(held.at[r], dst.at[r], out_sems.at[n]),
            )
        )
    for come, go in copies:
        come.start()
    for come, go in copies:
        come.wait()
        go.start()
    for come, go in copies:
        go.wait()


def body(layer_inputs, queries, key_values, out_grads, lengths, task_weights):
    hbm = pl.BlockSpec(memory_space=pl.ANY)
    wide = KVH * PAIR
    results = (
        jax.ShapeDtypeStruct((BLK, wide), F32),
        jax.ShapeDtypeStruct((BLK, wide), BF16),
    )
    fisher, merged = pl.pallas_call(
        step_kernel,
        out_shape=results,
        in_specs=[hbm] * 5 + [pl.BlockSpec(memory_space=pltpu.SMEM)],
        out_specs=(hbm, hbm),
        scratch_shapes=[
            pltpu.VMEM((TOK // 32, wide), BF16),
            pltpu.VMEM((TOK, PAIR), BF16),
            pltpu.VMEM((TOK, PAIR), BF16),
            pltpu.VMEM((TOK, BLK), BF16),
            pltpu.VMEM((BLK, wide), BF16),
            pltpu.VMEM((TOK, PAIR), BF16),
            pltpu.VMEM((2, 3, BLK, BLK), F32),
            pltpu.VMEM((2, 3, BLK, BLK), F32),
            pltpu.VMEM((TOK, PAIR), F32),
            pltpu.VMEM((TOK, PAIR), BF16),
            pltpu.VMEM((4, 3, OWN, PAIR), BF16),
            pltpu.VMEM((2, 2, 3 * HD, 2 * BLK), BF16),
            pltpu.VMEM((KVH, 2, 2 * BLK, PAIR), BF16),
            pltpu.VMEM((8, BLK, PAIR), F32),
            pltpu.VMEM((8, 2, HD, PAIR), BF16),
            pltpu.VMEM((8, 2, HD, PAIR), BF16),
            pltpu.VMEM((8, 2, HD, PAIR), BF16),
            pltpu.VMEM((8, 3, 2, 32, PAIR), BF16),
            pltpu.VMEM((KVH, BLK, PAIR), BF16),
            pltpu.SemaphoreType.DMA((TURNS,)),
            pltpu.SemaphoreType.DMA((SEMS,)),
            pltpu.SemaphoreType.DMA((8,)),
        ],
        compiler_params=pltpu.CompilerParams(collective_id=0, has_side_effects=True),
        name="step",
    )(key_values[0], queries[0], out_grads[0], layer_inputs[0], task_weights[0], lengths)
    fisher, merged = pl.pallas_call(
        write_kernel,
        out_shape=results,
        in_specs=[hbm, hbm],
        out_specs=(hbm, hbm),
        scratch_shapes=[
            pltpu.VMEM((BLK, wide), F32),
            pltpu.VMEM((BLK, wide), BF16),
            pltpu.SemaphoreType.DMA((8,)),
            pltpu.SemaphoreType.DMA((8,)),
        ],
        name="write",
    )(fisher, merged)
    return fisher[None], merged


def solution(mesh):
    placed = (
        P("task", None, "col"),
        P("task", None, "col"),
        P("task", "col", None),
        P("task", None, "col"),
        P("task", None),
        P("task", "col", None),
    )
    return jax.shard_map(
        body,
        mesh=mesh,
        in_specs=placed,
        out_specs=(P("task", "col", None), P("col", None)),
        check_vma=False,
    )
```

```python
import functools

import jax
import jax.numpy as jnp
from jax import lax
from jax.experimental import pallas as pl
from jax.experimental.pallas import tpu as pltpu
from jax.sharding import PartitionSpec as P

MESH = pl.DeviceIdType.MESH
F32, BF16 = jnp.float32, jnp.bfloat16
KVH = 8
HD = 128
PAIR = 2 * HD
TOK = 1024
BLK = 256
OWN = BLK // 4
CUT = 48
REST = 2 * OWN - CUT
EPS = 1e-06
NEGATIVE = -1e30
TURNS = 24
SEMS = 96


class Where:
    def __init__(self):
        self.task, self.col = lax.axis_index("task"), lax.axis_index("col")
        self.y, self.core = self.task // 2, self.task % 2
        self.z, self.x = self.col // 4, self.col % 4

    def along_x(self, by):
        return (self.task, self.z * 4 + (self.x + by + 4) % 4)

    def along_z(self, by):
        return (self.task, ((self.z + by + 8) % 8) * 4 + self.x)

    def along_y(self, by, across=False):
        core = 1 - self.core if across else self.core
        return (((self.y + by) % 4) * 2 + core, self.col)

    def other_core(self):
        return (self.y * 2 + 1 - self.core, self.col)


def meet(devices):
    barrier = pltpu.get_barrier_semaphore()
    for device in devices:
        pl.semaphore_signal(barrier, inc=1, device_id=device, device_id_type=MESH)
    pl.semaphore_wait(barrier, len(devices))


class Sender:
    def __init__(self, send_sems, recv_sems):
        self.send_sems, self.recv_sems = send_sems, recv_sems
        self.copies, self.used = [], 0

    def fresh(self):
        self.used += 1
        assert self.used <= SEMS
        return self.recv_sems.at[self.used - 1]

    def start(self, src, dst, device, recv_sem=None):
        at = len(self.copies)
        if at >= TURNS:
            self.copies[at - TURNS].wait_send()
        copy = pltpu.make_async_remote_copy(
            src_ref=src,
            dst_ref=dst,
            send_sem=self.send_sems.at[at % TURNS],
            recv_sem=self.fresh() if recv_sem is None else recv_sem,
            device_id=device,
            device_id_type=MESH,
        )
        copy.start()
        self.copies.append(copy)
        return copy

    def arrived(self, ref, recv_sem):
        pltpu.make_async_remote_copy(
            src_ref=ref,
            dst_ref=ref,
            send_sem=self.send_sems.at[0],
            recv_sem=recv_sem,
            device_id=(0, 0),
            device_id_type=MESH,
        ).wait_recv()

    def finish(self):
        for copy in self.copies[-TURNS:]:
            copy.wait_send()


def bounds(lengths_ref):
    ends, end = [], 0
    for s in range(4):
        end = end + lengths_ref[0, s]
        ends.append(end)
    return ends


def dot_nt(a, b):
    return lax.dot_general(a, b, (((1,), (1,)), ((), ())), preferred_element_type=F32)


def step_kernel(
    kv_hbm,
    q_hbm,
    og_hbm,
    x_hbm,
    w_hbm,
    len_ref,
    fisher_out,
    merged_out,
    kv_ref,
    q_ref,
    og_ref,
    x_ref,
    w_ref,
    kv,
    score,
    slope,
    acc,
    p_ref,
    rs_in,
    xm,
    g,
    fb,
    ps,
    pr,
    ys,
    yr,
    mb,
    send_sems,
    recv_sems,
    local_sems,
):
    at = Where()
    send = Sender(send_sems, recv_sems)
    x, z, y, core = at.x, at.z, at.y, at.core

    loads = []
    for n, (src, dst) in enumerate(
        ((kv_hbm, kv_ref), (q_hbm, q_ref), (og_hbm, og_ref), (x_hbm, x_ref), (w_hbm, w_ref))
    ):
        copy = pltpu.make_async_copy(src, dst, local_sems.at[n])
        copy.start()
        loads.append(copy)
    meet(
        [at.along_z(k) for k in (4, 3, 5, 2, 6, 1, 7)]
        + [at.along_y(k) for k in (2, 1, 3)]
        + [at.along_y(k, True) for k in (2, 1, 3)]
        + [at.along_x(2), at.along_x(1), at.along_x(-1), at.other_core()]
    )

    def rows(z, x):
        return pl.ds(pl.multiple_of(z * 128 + x * 32, 32), 32)

    def columns(h):
        return pl.ds(pl.multiple_of(h * PAIR, PAIR), PAIR)

    loads[0].wait()
    own = pltpu.make_async_copy(kv_ref.at[:, columns(z)], kv.at[rows(z, x)], local_sems.at[5])
    own.start()
    steps = (1, 7, 2, 6, 3, 5, 4)
    spare = {k: send.fresh() for k in steps}
    arrive = {
        k: send.start(kv_ref.at[:, columns((z + k) % 8)], kv.at[rows(z, x)], at.along_z(k), spare[k])
        for k in steps
    }
    spare = list(spare.values())
    spread = []

    def spread_block(z):
        block = kv.at[rows(z, x)]
        for by in (1, -1, 2):
            spare.append(send.fresh())
            spread.append(send.start(block, block, at.along_x(by), spare[-1]))

    own.wait()
    spread_block(z)
    for k in steps:
        arrive[k].wait_recv()
        spread_block((z + 8 - k) % 8)
    for copy in loads[1:3]:
        copy.wait()
    for copy in spread:
        copy.wait_recv()

    factor = HD**-0.5
    ends = bounds(len_ref)
    blocks = TOK // BLK

    def piece_of(j, by):
        return pl.ds(pl.multiple_of(j * BLK + ((x + by + 4) % 4) * OWN, OWN), OWN)

    block_sems = [send.fresh() for j in range(blocks)]

    def send_block(j):
        for by in (2, 1, 3):
            send.start(p_ref.at[piece_of(j, by)], rs_in.at[j, by - 1], at.along_x(by), block_sems[j])

    for i in reversed(range(blocks)):
        queries = pl.ds(i * BLK, BLK)
        low = max(0, i - 2)
        token = i * BLK + lax.broadcasted_iota(jnp.int32, (1, BLK), 1)
        opening = jnp.zeros_like(token)
        for s in range(3):
            opening = jnp.where(token >= ends[s], ends[s], opening)
        heads_in = [
            (q_ref[queries, m * HD : m * HD + HD], og_ref[queries, m * HD : m * HD + HD])
            for m in range(2)
        ]
        both_queries = jnp.concatenate([query for query, cot in heads_in], axis=0)
        both_cots = jnp.concatenate([cot for query, cot in heads_in], axis=0)
        highest = [jnp.full((1, BLK), NEGATIVE, F32)] * 2
        for j in range(low, i + 1):
            key = kv[pl.ds(j * BLK, BLK), 0:HD]
            place = j * BLK + lax.broadcasted_iota(jnp.int32, (BLK, BLK), 0)
            allowed = place >= opening
            if j == i:
                allowed = allowed & (place <= token)
            for m in range(2):
                s = jnp.where(allowed, dot_nt(key, heads_in[m][0]) * factor, NEGATIVE)
                score[m, j - low] = s
                highest[m] = jnp.maximum(highest[m], jnp.max(s, axis=0, keepdims=True))
        total = [jnp.zeros((1, BLK), F32)] * 2
        weighed = [jnp.zeros((1, BLK), F32)] * 2
        for j in range(low, i + 1):
            value = kv[pl.ds(j * BLK, BLK), HD:PAIR]
            for m in range(2):
                e = jnp.exp(score[m, j - low] - highest[m])
                score[m, j - low] = e
                d = dot_nt(value, heads_in[m][1])
                slope[m, j - low] = d
                total[m] = total[m] + jnp.sum(e, axis=0, keepdims=True)
                weighed[m] = weighed[m] + jnp.sum(e * d, axis=0, keepdims=True)
        inverse = [1.0 / total[m] for m in range(2)]
        offset = [weighed[m] * inverse[m] for m in range(2)]
        for j in range(low, i + 1):
            to = pl.ds(j * BLK, BLK)
            chances = [score[m, j - low] * inverse[m] for m in range(2)]
            slopes = [
                (chances[m] * (slope[m, j - low] - offset[m])).astype(BF16) for m in range(2)
            ]
            chances = [p.astype(BF16) for p in chances]
            dk = jnp.dot(jnp.concatenate(slopes, axis=1), both_queries, preferred_element_type=F32)
            dv = jnp.dot(jnp.concatenate(chances, axis=1), both_cots, preferred_element_type=F32)
            if i == min(blocks - 1, j + 2):
                acc[to, 0:HD] = dk
                acc[to, HD:PAIR] = dv
            else:
                acc[to, 0:HD] += dk
                acc[to, HD:PAIR] += dv
        done = pl.ds(i * BLK, BLK)
        p_ref[done, 0:HD] = (acc[done, 0:HD] * factor).astype(BF16)
        p_ref[done, HD:PAIR] = acc[done, HD:PAIR].astype(BF16)
        send_block(i)

    loads[3].wait()
    starts = [0] + ends[:3]
    for hf in range(2):
        o = 2 * BLK * hf
        early = [x_ref[o + OWN * q : o + OWN * q + CUT] for q in range(4)]
        late = []
        for q in range(4):
            late.append(x_ref[o + OWN * q + CUT : o + OWN * q + OWN])
            late.append(x_ref[o + BLK + OWN * q : o + BLK + OWN * q + OWN])
        turned = jnp.concatenate(early + late, axis=0).T
        pos = lax.broadcasted_iota(jnp.int32, (1, 2 * BLK), 1)
        token = jnp.zeros_like(pos)
        for q in range(4):
            token = jnp.where(pos >= CUT * q, pos - CUT * q + OWN * q, token)
        for q in range(4):
            base = 4 * CUT + REST * q
            token = jnp.where(pos >= base, pos - base + CUT + OWN * q, token)
            base += OWN - CUT
            token = jnp.where(pos >= base, pos - base + BLK + OWN * q, token)
        token = token + o
        for n in range(3):
            s = hf + n
            inside = jnp.where((token >= starts[s]) & (token < ends[s]), 1.0, 0.0).astype(BF16)
            masked = turned * inside
            for rb in range(2):
                xm[rb, hf, n * HD : (n + 1) * HD, :] = masked[rb * HD : (rb + 1) * HD]
    loads[4].wait()

    def cut_rows(q):
        return pl.ds(pl.multiple_of(CUT * (q % 4), CUT), CUT)

    def rest_rows(q, skip=0, length=REST):
        return pl.ds(pl.multiple_of(4 * CUT + REST * (q % 4) + skip, 16), length)

    def settle(j):
        send.arrived(rs_in.at[j], block_sems[j])
        summed = p_ref[piece_of(j, 0), :].astype(F32)
        for by in range(3):
            summed = summed + rs_in[j, by].astype(F32)
        summed = summed.astype(BF16)
        if j % 2 == 0:
            g[z, j // 2, cut_rows(x), :] = summed[:CUT]
            g[z, j // 2, rest_rows(x, 0, OWN - CUT), :] = summed[CUT:]
        else:
            g[z, j // 2, rest_rows(x, OWN - CUT, OWN), :] = summed

    def around_copy(piece, way):
        return send.start(piece, piece, at.along_x(way), spare.pop(0) if spare else None)

    class Ring:
        def __init__(self, h, sems=None):
            self.h, self.sems = h, sems
            own = g.at[h, :, rest_rows(x)]
            if sems is None:
                self.up = around_copy(own, 1)
                self.down = around_copy(own, -1)

        def come(self, name):
            if self.sems is None:
                getattr(self, name).wait_recv()
            else:
                send.arrived(g.at[self.h, :, rest_rows(x)], self.sems[name])

        def pass_on(self):
            self.come("up")
            self.up2 = around_copy(g.at[self.h, 0, rest_rows(x + 3)], 1)
            self.come("down")
            self.down2 = around_copy(g.at[self.h, 1, rest_rows(x + 1)], -1)

        def end(self):
            self.up2.wait_recv()
            self.down2.wait_recv()

    def head(k):
        return (z + k + 8) % 8

    def send_rest(h, way):
        piece = g.at[h, :, rest_rows(x)]
        return send.start(piece, piece, at.along_z(way))

    def send_cut(h, hf, way):
        piece = g.at[h, hf, 0 : 4 * CUT]
        return send.start(piece, piece, at.along_z(way))

    heads = [0, -1, 1, -2, 2, -3, 3, 4]

    def fisher_rows(slot, h, rb):
        a = jnp.dot(xm[rb, 0], g[h, 0], preferred_element_type=F32)
        b = jnp.dot(xm[rb, 1], g[h, 1], preferred_element_type=F32)
        g0, g3 = a[:HD], b[2 * HD :]
        g1, g2 = a[HD : 2 * HD] + b[:HD], a[2 * HD :] + b[HD : 2 * HD]
        f = g0 * g0 + g1 * g1 + g2 * g2 + g3 * g3
        fb[slot, pl.ds(pl.multiple_of(rb * HD, HD), HD), :] = f
        return f

    def weights(h, rb):
        return w_ref[pl.ds(pl.multiple_of(rb * HD, HD), HD), columns(h)].astype(F32)

    pair, over_y, merged_y, merged_core = {}, {}, {}, {}

    def compute_other(slot):
        h = head(heads[slot])
        rb = 1 - core
        f = fisher_rows(slot, h, rb)
        ps[slot, 0] = (f * weights(h, rb)).astype(BF16)
        ps[slot, 1] = f.astype(BF16)
        pair[slot] = send.start(ps.at[slot], pr.at[slot], at.other_core())

    def compute_own(slot):
        h = head(heads[slot])
        fisher_rows(slot, h, core)
        pltpu.make_async_copy(fb.at[slot], fisher_out.at[:, columns(h)], local_sems.at[6]).start()

    def sum_pair(slot):
        h = head(heads[slot])
        pair[slot].wait_recv()
        f = fb[slot, pl.ds(pl.multiple_of(core * HD, HD), HD), :]
        ys[slot, 0] = (f * weights(h, core) + pr[slot, 0].astype(F32)).astype(BF16)
        ys[slot, 1] = (f + pr[slot, 1].astype(F32)).astype(BF16)
        over_y[slot] = send.fresh()
        for k in (2, 1, 3):
            r = pl.ds(pl.multiple_of(((y + k) % 4) * 32, 32), 32)
            send.start(ys.at[slot, :, r], yr.at[slot, k - 1], at.along_y(k), over_y[slot])

    def divide(slot):
        h = head(heads[slot])
        send.arrived(yr.at[slot], over_y[slot])
        r = pl.ds(pl.multiple_of(y * 32, 32), 32)
        sums = ys[slot, :, r, :].astype(F32)
        for k in range(3):
            sums = sums + yr[slot, k].astype(F32)
        to = pl.ds(pl.multiple_of(core * HD + y * 32, 32), 32)
        mb[h, to, :] = (sums[0] / (sums[1] + EPS)).astype(BF16)
        piece = mb.at[h, to]
        merged_y[slot] = send.fresh()
        for k in (2, 1, 3):
            send.start(piece, piece, at.along_y(k), merged_y[slot])
        if slot == 7:
            for k in (2, 1, 3):
                send.start(piece, piece, at.along_y(k, True), merged_y[slot])
            send.start(piece, piece, at.other_core(), merged_y[slot])

    def share(slot):
        h = head(heads[slot])
        send.arrived(mb.at[h, 0 : 224 if slot == 7 else 96], merged_y[slot])
        if slot < 7:
            piece = mb.at[h, pl.ds(pl.multiple_of(core * HD, HD), HD)]
            merged_core[slot] = send.start(piece, piece, at.other_core())

    def close(slot):
        h = head(heads[slot])
        if slot < 7:
            merged_core[slot].wait_recv()
        pltpu.make_async_copy(mb.at[h], merged_out.at[:, columns(h)], local_sems.at[7]).start()

    rings = {}
    rest = {}
    rest_first = {"up": send.fresh(), "down": send.fresh()}
    ways = (("up", 1), ("down", -1))

    def rest_arrives(name, k):
        if k == 1:
            send.arrived(g.at[z, :, rest_rows(x)], rest_first[name])
        else:
            rest[name].wait_recv()

    def rest_hop(k):
        if k < 4:
            rest_arrives("up", k)
            if k < 3:
                rest["up"] = send_rest(head(-k), 1)
        rest_arrives("down", k)
        if k < 4:
            rest["down"] = send_rest(head(k), -1)

    def around(slot):
        rings[slot] = Ring(head(heads[slot]))

    cut = {}

    def cut_hop(k, hf):
        last_up, last_down = (4, 3) if hf == 0 else (3, 4)
        if k <= last_up:
            cut["up", hf].wait_recv()
            if k < last_up:
                cut["up", hf] = send_cut(head(-k), hf, 1)
        if k <= last_down:
            cut["down", hf].wait_recv()
            if k < last_down:
                cut["down", hf] = send_cut(head(k), hf, -1)

    def further(slot):
        rings[slot].pass_on()
        if slot + 2 < 8:
            around(slot + 2)

    cut_ring = {}
    ring_first = {"up": spare.pop(0), "down": spare.pop(0)}
    rings[0] = Ring(z, ring_first)
    for hf in (1, 0):
        settle(2 * hf + 1)
        settle(2 * hf)
        for name, way in ways:
            piece = g.at[z, hf, cut_rows(x)]
            cut_ring[name, hf] = around_copy(piece, way)
        for name, way in ways:
            piece = g.at[z, hf, rest_rows(x)]
            send.start(piece, piece, at.along_z(way), rest_first[name])
        for name, way in ways:
            piece = g.at[z, hf, rest_rows(x)]
            send.start(piece, piece, at.along_x(way), ring_first[name])
    cut_ring["up", 1].wait_recv()
    far_up = around_copy(g.at[z, 1, cut_rows(x + 3)], 1)
    cut_ring["down", 0].wait_recv()
    far_down = around_copy(g.at[z, 0, cut_rows(x + 1)], -1)
    rest_hop(1)
    around(1)
    further(0)
    cut_ring["down", 1].wait_recv()
    far_up.wait_recv()
    for name, way in ways:
        cut[name, 1] = send_cut(z, 1, way)
    cut_ring["up", 0].wait_recv()
    far_down.wait_recv()
    for name, way in ways:
        cut[name, 0] = send_cut(z, 0, way)
    rest_hop(2)
    further(1)
    for slot in range(8):
        rings[slot].end()
        compute_other(slot)
        compute_own(slot)
        if slot + 2 < 8:
            further(slot + 2)
        if slot in (0, 2):
            rest_hop(slot // 2 + 3)
        if slot % 2 == 0 and slot < 7:
            cut_hop(slot // 2 + 1, 1)
            cut_hop(slot // 2 + 1, 0)
        sum_pair(slot)
        if slot >= 2:
            divide(slot - 2)
        if slot >= 4:
            share(slot - 4)
    divide(6)
    share(4)
    close(0)
    close(1)
    divide(7)
    close(2)
    share(5)
    close(3)
    close(4)
    share(6)
    share(7)
    for slot in (7, 5, 6):
        close(slot)
    send.finish()
    pltpu.make_async_copy(fb, fb, local_sems.at[6]).wait()
    pltpu.make_async_copy(mb, mb, local_sems.at[7]).wait()


def write_kernel(fisher_ref, merged_ref, fisher_out, merged_out, fisher, merged, in_sems, out_sems):
    copies = []
    for n in range(8):
        src, held, dst = (
            (fisher_ref, fisher, fisher_out) if n < 4 else (merged_ref, merged, merged_out)
        )
        r = pl.ds((n % 4) * (BLK // 4), BLK // 4)
        copies.append(
            (
                pltpu.make_async_copy(src.at[r], held.at[r], in_sems.at[n]),
                pltpu.make_async_copy(held.at[r], dst.at[r], out_sems.at[n]),
            )
        )
    for come, go in copies:
        come.start()
    for come, go in copies:
        come.wait()
        go.start()
    for come, go in copies:
        go.wait()


def body(layer_inputs, queries, key_values, out_grads, lengths, task_weights):
    hbm = pl.BlockSpec(memory_space=pl.ANY)
    wide = KVH * PAIR
    results = (
        jax.ShapeDtypeStruct((BLK, wide), F32),
        jax.ShapeDtypeStruct((BLK, wide), BF16),
    )
    fisher, merged = pl.pallas_call(
        step_kernel,
        out_shape=results,
        in_specs=[hbm] * 5 + [pl.BlockSpec(memory_space=pltpu.SMEM)],
        out_specs=(hbm, hbm),
        scratch_shapes=[
            pltpu.VMEM((TOK // 32, wide), BF16),
            pltpu.VMEM((TOK, PAIR), BF16),
            pltpu.VMEM((TOK, PAIR), BF16),
            pltpu.VMEM((TOK, BLK), BF16),
            pltpu.VMEM((BLK, wide), BF16),
            pltpu.VMEM((TOK, PAIR), BF16),
            pltpu.VMEM((2, 3, BLK, BLK), F32),
            pltpu.VMEM((2, 3, BLK, BLK), F32),
            pltpu.VMEM((TOK, PAIR), F32),
            pltpu.VMEM((TOK, PAIR), BF16),
            pltpu.VMEM((4, 3, OWN, PAIR), BF16),
            pltpu.VMEM((2, 2, 3 * HD, 2 * BLK), BF16),
            pltpu.VMEM((KVH, 2, 2 * BLK, PAIR), BF16),
            pltpu.VMEM((8, BLK, PAIR), F32),
            pltpu.VMEM((8, 2, HD, PAIR), BF16),
            pltpu.VMEM((8, 2, HD, PAIR), BF16),
            pltpu.VMEM((8, 2, HD, PAIR), BF16),
            pltpu.VMEM((8, 3, 2, 32, PAIR), BF16),
            pltpu.VMEM((KVH, BLK, PAIR), BF16),
            pltpu.SemaphoreType.DMA((TURNS,)),
            pltpu.SemaphoreType.DMA((SEMS,)),
            pltpu.SemaphoreType.DMA((8,)),
        ],
        compiler_params=pltpu.CompilerParams(collective_id=0, has_side_effects=True),
        name="step",
    )(key_values[0], queries[0], out_grads[0], layer_inputs[0], task_weights[0], lengths)
    fisher, merged = pl.pallas_call(
        write_kernel,
        out_shape=results,
        in_specs=[hbm, hbm],
        out_specs=(hbm, hbm),
        scratch_shapes=[
            pltpu.VMEM((BLK, wide), F32),
            pltpu.VMEM((BLK, wide), BF16),
            pltpu.SemaphoreType.DMA((8,)),
            pltpu.SemaphoreType.DMA((8,)),
        ],
        name="write",
    )(fisher, merged)
    return fisher[None], merged


def solution(mesh):
    placed = (
        P("task", None, "col"),
        P("task", None, "col"),
        P("task", "col", None),
        P("task", None, "col"),
        P("task", None),
        P("task", "col", None),
    )
    return jax.shard_map(
        body,
        mesh=mesh,
        in_specs=placed,
        out_specs=(P("task", "col", None), P("col", None)),
        check_vma=False,
    )
```
